128 devices in a mesh: gx: 16 (over y_hi, z, core), gy: 8 (over y_lo, x).
Axes of the slice: x: 4, y: 4 (y_hi: 2, y_lo: 2; y = y_hi * 2 + y_lo), z: 4, core: 2. Of those that a mesh axis runs over, the one named last changes fastest.
Arguments:
- features: bfloat16 [32, 128, 64, 128], P(None, 'gx', 'gy'), may hold values from -6 to 6
- occupancy: int32 [16, 8, 16], replicated, may hold values 0 or 1
- weight_one: bfloat16 [32, 3, 3, 3, 32], replicated, may hold values from -0.21875 to 0.21875
- bias_one: float32 [32], replicated, may hold values from -3 to 3
- weight_two: bfloat16 [32, 3, 3, 3, 32], replicated, may hold values from -0.21875 to 0.21875
- bias_two: float32 [32], replicated, may hold values from -3 to 3
- grad_pooled: bfloat16 [32, 64, 32, 64], P(None, 'gx', 'gy'), may hold values from -24 to 24
- pool_choice: int32 [32, 64, 32, 64], P(None, 'gx', 'gy'), may hold values from 0 to 7
Outputs:
- grad_input: bfloat16 [32, 128, 64, 128], P(None, 'gx', 'gy')
- grad_weight_one: float32 [32, 3, 3, 3, 32], replicated
- grad_bias_one: float32 [32], replicated
- grad_weight_two: float32 [32, 3, 3, 3, 32], replicated
- grad_bias_two: float32 [32], replicated
The draws below stay inside these ranges and needn't reach their ends.
All inputs are finite; a program needn't handle non-finite values.
Results may differ from the reference program's by a relative error of at most 0.035.
The reference program's roundings to bfloat16 on the way (of `masked`, `hidden`, `upstream`, `delta_two` and `delta_one`) count: a program that leaves them out, or rounds other values in their place, can miss the bound.
Values may be sent and summed in bfloat16 or wider, within the bound.
No kernel may reach another device: no remote copies, remote signals or barrier semaphores. Data moves between devices by JAX's collectives and lax.ppermute only.
A program may use at most 64 MiB of HBM per device.

```python
import math
import jax
import jax.numpy as jnp
from jax import lax

C = 32
NX = 128
NY = 64
NZ = 128


def touch_ends(array, stream_key, least, high):
    place = [jax.random.randint(jax.random.fold_in(stream_key, axis), (), 0, length) for axis, length in enumerate(array.shape)]
    longest = array.shape.index(max(array.shape))
    next_to = place[:longest] + [(place[longest] + 1) % array.shape[longest]] + place[longest + 1:]
    return array.at[tuple(place)].set(least).at[tuple(next_to)].set(high)


def shard_levels(key, extent, shards, least, top_value):
    def one(dim, blocks):
        heights = jax.random.uniform(jax.random.fold_in(jax.random.fold_in(key, 6), dim), (blocks,), jnp.float32, least / len(shards), top_value / len(shards))
        return jnp.repeat(jnp.exp(heights), extent[dim] // blocks).reshape((-1,) + (1,) * (len(extent) - dim - 1))

    gain = one(*shards[0])
    for cut in shards[1:]:
        gain = gain * one(*cut)
    return gain


def noise(own_key, extent, scale, most, split=(), held_as=jnp.bfloat16):
    drawn = scale * jax.random.normal(own_key, extent, jnp.float32)
    if split:
        drawn = drawn * shard_levels(own_key, extent, split, -0.22, 0.18)
    return jnp.clip(drawn, -most, most).astype(held_as)


def setup_inputs(seed: int = 0) -> dict:
    key_of = jax.random.split(jax.random.key(seed), 9)
    return {
        "features": noise(key_of[0], (C, NX, NY, NZ), 1.0, 6.0, ((1, 16), (2, 8))),
        "occupancy": touch_ends((jax.random.randint(key_of[1], (NX // 8, NY // 8, NZ // 8), 0, 4) < 3).astype(jnp.int32), jax.random.fold_in(key_of[1], 1), 0, 1),
        "weight_one": noise(key_of[2], (C, 3, 3, 3, C), (27 * C) ** -0.5, 0.21875),
        "bias_one": noise(key_of[3], (C,), 0.5, 3.0, (), jnp.float32),
        "weight_two": noise(key_of[4], (C, 3, 3, 3, C), (27 * C) ** -0.5, 0.21875),
        "bias_two": noise(key_of[5], (C,), 0.5, 3.0, (), jnp.float32),
        "grad_pooled": noise(key_of[6], (C, NX // 2, NY // 2, NZ // 2), 4.0, 24.0, ((1, 16), (2, 8))),
        "pool_choice": touch_ends(jax.random.randint(key_of[7], (C, NX // 2, NY // 2, NZ // 2), 0, 8), jax.random.fold_in(key_of[7], 1), 0, 7).astype(jnp.int32),
    }


def convolve(inputs, weight):
    kernel = weight.transpose(0, 4, 1, 2, 3)
    result = lax.conv_general_dilated(inputs[None], kernel, (1, 1, 1), [(1, 1), (1, 1), (1, 1)], dimension_numbers=('NCDHW', 'OIDHW', 'NCDHW'), precision=lax.Precision.HIGHEST)
    return result[0]

def expand(field, factor):
    return jnp.repeat(jnp.repeat(jnp.repeat(field, factor, axis=-3), factor, axis=-2), factor, axis=-1)

def reference(features, occupancy, weight_one, bias_one, weight_two, bias_two, grad_pooled, pool_choice):
    mask = expand(occupancy, 8).astype(jnp.float32)
    masked = features.astype(jnp.float32) * mask
    first_f = weight_one.astype(jnp.float32)
    second_f = weight_two.astype(jnp.float32)
    conv_one, pull_one = jax.vjp(convolve, masked, first_f)
    pre_one = conv_one + bias_one[:, None, None, None]
    hidden = (jnp.maximum(pre_one, 0.0) * mask).astype(jnp.bfloat16)
    conv_two, pull_two = jax.vjp(convolve, hidden.astype(jnp.float32), second_f)
    pre_two = conv_two + bias_two[:, None, None, None]
    spread = expand(grad_pooled.astype(jnp.float32), 2)
    chosen = expand(pool_choice, 2)
    xpos = jnp.arange(NX, dtype=jnp.int32)[:, None, None] % 2
    ypos = jnp.arange(NY, dtype=jnp.int32)[None, :, None] % 2
    zpos = jnp.arange(NZ, dtype=jnp.int32)[None, None, :] % 2
    code = 4 * xpos + 2 * ypos + zpos
    upstream = jnp.where(chosen == code[None], spread, 0.0)
    delta_two = (upstream * (pre_two > 0).astype(jnp.float32) * mask).astype(jnp.bfloat16)
    back_one, grad_w_two = pull_two(delta_two.astype(jnp.float32))
    delta_one = (back_one * (pre_one > 0).astype(jnp.float32) * mask).astype(jnp.bfloat16)
    back_input, grad_w_one = pull_one(delta_one.astype(jnp.float32))
    scale = 1.0 / math.sqrt(NX * NY * NZ)
    grad_input = (back_input * mask).astype(jnp.bfloat16)
    grad_b_one = lax.optimization_barrier(jnp.sum(delta_one.astype(jnp.float32), axis=(1, 2, 3))) * scale
    grad_b_two = lax.optimization_barrier(jnp.sum(delta_two.astype(jnp.float32), axis=(1, 2, 3))) * scale
    return (grad_input, grad_w_one * scale, grad_b_one, grad_w_two * scale, grad_b_two)
```

```python
import math

import jax
import jax.numpy as jnp
from jax import lax
from jax.sharding import PartitionSpec as P


def padded_2(x, sides, width):
    for axis, dim in sides:
        devices, length = (lax.axis_size(axis), x.shape[dim])
        up = [(i, (i + 1) % devices) for i in range(devices - 1)]
        down = [(j, i) for i, j in up]
        last = lax.slice_in_dim(x, length - width, length, axis=dim)
        first = lax.slice_in_dim(x, 0, width, axis=dim)
        before = lax.ppermute(last, axis, up)
        after = lax.ppermute(first, axis, down)
        x = jnp.concatenate([before, x, after], axis=dim)
    return x


def together(arrays, axes):
    devices = 1
    for axis in axes:
        devices *= lax.axis_size(axis)
    flat = jnp.concatenate([a.reshape(-1) for a in arrays])
    rows = -(-flat.size // (devices * 128))
    flat = jnp.pad(flat, (0, devices * rows * 128 - flat.size)).astype(jnp.bfloat16)
    parts = lax.all_to_all(flat.reshape(devices, rows, 128), axes, 0, 0, tiled=True)
    mine = jnp.sum(parts.astype(jnp.float32), axis=0).astype(jnp.bfloat16)
    spread = jnp.broadcast_to(mine[None], (devices, rows, 128))
    summed = lax.all_to_all(spread, axes, 0, 0, tiled=True).reshape(-1).astype(jnp.float32)
    outs, at = [], 0
    for a in arrays:
        outs.append(summed[at : at + a.size].reshape(a.shape))
        at += a.size
    return tuple(outs)


def depth_stack(padded):
    depth = padded.shape[3]
    framed = jnp.pad(padded, ((0, 0), (0, 0), (0, 0), (1, 1)))
    return jnp.concatenate(
        [framed[..., 0:depth], framed[..., 1 : depth + 1], framed[..., 2 : depth + 2]], axis=0
    )


def convolve(stacked, weight):
    width_x = stacked.shape[1] - 2
    width_y = stacked.shape[2] - 2
    channels = weight.shape[0]
    total = None
    for row_off in range(3):
        for col_off in range(3):
            kernel = weight[:, row_off, col_off].reshape(channels, -1)
            window = stacked[:, row_off : row_off + width_x, col_off : col_off + width_y, :]
            term = jnp.einsum("ok,kxyz->oxyz", kernel, window, preferred_element_type=jnp.float32)
            total = term if total is None else total + term
    return total


def weight_grad(upstream, stacked):
    width_x = upstream.shape[1]
    width_y = upstream.shape[2]
    channels = upstream.shape[0]
    blocks = []
    for row_off in range(3):
        column_parts = []
        for col_off in range(3):
            window = stacked[:, row_off : row_off + width_x, col_off : col_off + width_y, :]
            part = jnp.einsum("oxyz,kxyz->ok", upstream, window, preferred_element_type=jnp.float32)
            column_parts.append(part.reshape(channels, 3, -1))
        blocks.append(jnp.stack(column_parts, axis=1))
    return jnp.stack(blocks, axis=1)


def flipped(weight):
    return jnp.flip(weight, (1, 2, 3)).transpose(4, 1, 2, 3, 0)


def expand(field, factor):
    return jnp.repeat(
        jnp.repeat(jnp.repeat(field, factor, axis=-3), factor, axis=-2), factor, axis=-1
    )


def body(features, occupancy, weight_one, bias_one, weight_two, bias_two, grad_pooled, pool_choice):
    cells_x = features.shape[1]
    cells_y = features.shape[2]
    cells_z = features.shape[3]
    brick_x = cells_x // 8
    brick_y = cells_y // 8
    padded_flags = jnp.pad(occupancy, ((1, 1), (1, 1), (0, 0)))
    corner_x = lax.axis_index("gx") * brick_x
    corner_y = lax.axis_index("gy") * brick_y
    flag_window = lax.dynamic_slice(
        padded_flags,
        (corner_x, corner_y, jnp.int32(0)),
        (brick_x + 2, brick_y + 2, occupancy.shape[2]),
    )
    cell_flags = expand(flag_window, 8).astype(jnp.float32)
    mask_inner = cell_flags[8 : 8 + cells_x, 8 : 8 + cells_y]
    masked = (features.astype(jnp.float32) * mask_inner).astype(jnp.bfloat16)
    input_padded = padded_2(masked, (("gx", 1), ("gy", 2)), 1)
    input_stack = depth_stack(input_padded)
    pre_one = convolve(input_stack, weight_one) + bias_one[:, None, None, None]
    hidden = (jnp.maximum(pre_one, 0.0) * mask_inner).astype(jnp.bfloat16)
    hidden_padded = padded_2(hidden, (("gx", 1), ("gy", 2)), 1)
    hidden_stack = depth_stack(hidden_padded)
    pre_two = convolve(hidden_stack, weight_two) + bias_two[:, None, None, None]
    spread = expand(grad_pooled.astype(jnp.float32), 2)
    chosen = expand(pool_choice, 2)
    shape_cells = (cells_x, cells_y, cells_z)
    parity = (
        4 * (lax.broadcasted_iota(jnp.int32, shape_cells, 0) % 2)
        + 2 * (lax.broadcasted_iota(jnp.int32, shape_cells, 1) % 2)
        + lax.broadcasted_iota(jnp.int32, shape_cells, 2) % 2
    )
    upstream = jnp.where(chosen == parity[None], spread, 0.0)
    delta_two = (upstream * (pre_two > 0).astype(jnp.float32) * mask_inner).astype(jnp.bfloat16)
    local_w_two = weight_grad(delta_two, hidden_stack)
    local_b_two = jnp.sum(delta_two.astype(jnp.float32), axis=(1, 2, 3))
    delta_two_padded = padded_2(delta_two, (("gx", 1), ("gy", 2)), 1)
    back_one = convolve(depth_stack(delta_two_padded), flipped(weight_two))
    delta_one = (back_one * (pre_one > 0).astype(jnp.float32) * mask_inner).astype(jnp.bfloat16)
    local_w_one = weight_grad(delta_one, input_stack)
    local_b_one = jnp.sum(delta_one.astype(jnp.float32), axis=(1, 2, 3))
    summed_w_one, summed_b_one, summed_w_two, summed_b_two = together(
        (local_w_one, local_b_one, local_w_two, local_b_two), ("gx", "gy")
    )
    delta_one_padded = padded_2(delta_one, (("gx", 1), ("gy", 2)), 1)
    back_input = convolve(depth_stack(delta_one_padded), flipped(weight_one))
    grad_input = (back_input * mask_inner).astype(jnp.bfloat16)
    total_cells = cells_x * lax.axis_size("gx") * cells_y * lax.axis_size("gy") * cells_z
    scale = 1.0 / math.sqrt(total_cells)
    return (
        grad_input,
        summed_w_one * scale,
        summed_b_one * scale,
        summed_w_two * scale,
        summed_b_two * scale,
    )


def solution(mesh):
    placed = (
        P(None, "gx", "gy", None),
        P(),
        P(),
        P(),
        P(),
        P(),
        P(None, "gx", "gy", None),
        P(None, "gx", "gy", None),
    )
    return jax.shard_map(
        body,
        mesh=mesh,
        in_specs=placed,
        out_specs=(P(None, "gx", "gy", None), P(), P(), P(), P()),
        check_vma=False,
    )
```

```python
import math

import jax
import jax.numpy as jnp
from jax import lax
from jax.experimental import pallas as pl
from jax.experimental.pallas import tpu as pltpu
from jax.sharding import PartitionSpec as P

BF = jnp.bfloat16
F32 = jnp.float32
HALO = 4


def shift(v, axis, step):
    devices = lax.axis_size(axis)
    pairs = [(i, i + step) for i in range(devices) if 0 <= i + step < devices]
    return lax.ppermute(v, axis, pairs)


def toeplitz(kernel):
    k = kernel.transpose(3, 0, 1, 2, 4)
    zero = jnp.zeros_like(k[:, :, :, :1])
    lower = jnp.concatenate([k, zero], axis=3)
    upper = jnp.concatenate([zero, k], axis=3)
    chan = kernel.shape[0]
    return jnp.stack([lower, upper], axis=0).reshape(6 * chan, 12 * chan)


def flipped(weight):
    return jnp.flip(weight, (1, 2, 3)).transpose(4, 1, 2, 3, 0)


def section(own, xlow, xhigh, ylow, yhigh, pown, mask, w1, w2, f2, f1, b1, b2,
            out, parts, feat, pool, hid, two, one, ups, acc1, acc2):
    C, Z = 32, 128
    N = out.shape[0]
    H = HALO
    W = N + 2 * H
    Q = N // 2
    PW = Q + 2
    feat[H:H + N, H * C:(H + N) * C, :] = own[...]
    for k in range(H):
        for y in range(N):
            r = slice((H + y) * C, (H + y + 1) * C)
            feat[k, r, :] = xlow[k * N + y]
            feat[H + N + k, r, :] = xhigh[k * N + y]
    for x in range(W):
        for k in range(H):
            feat[x, k * C:(k + 1) * C, :] = ylow[x * H + k]
            feat[x, (H + N + k) * C:(H + N + k + 1) * C, :] = yhigh[x * H + k]
    pool[1:1 + Q, C:(1 + Q) * C, :] = pown[...]
    for y in range(Q):
        r = slice((1 + y) * C, (2 + y) * C)
        pool[0, r, :] = xlow[H * N + y]
        pool[1 + Q, r, :] = xhigh[H * N + y]
    for x in range(PW):
        pool[x, 0:C, :] = ylow[W * H + x]
        pool[x, (1 + Q) * C:(2 + Q) * C, :] = yhigh[W * H + x]
    row = lax.broadcasted_iota(jnp.int32, (Z, 2 * Z), 0)
    col = lax.broadcasted_iota(jnp.int32, (Z, 2 * Z), 1)
    spread = jnp.where(row == col // 2, 1.0, 0.0).astype(BF)
    for x in range(PW):
        ups[x] = jnp.dot(pool[x], spread, preferred_element_type=F32)

    lane = lax.broadcasted_iota(jnp.int32, (C, Z), 1)
    at_start = lane == 0
    at_end = lane == Z - 1
    odd = (lane % 2).astype(F32)

    def after(v):
        return jnp.where(at_start, 0.0, pltpu.roll(v, 1, 1))

    def before(v):
        return jnp.where(at_end, 0.0, pltpu.roll(v, Z - 1, 1))

    def conv(src, weight, width, write):
        def trip(i, carry):
            x = 2 * i
            for j in range(width // 2):
                y = 2 * j
                r = slice(y * C, (y + 4) * C)
                rows = [src[x + d, r, :] for d in range(4)]
                tile = jnp.concatenate(
                    [jnp.concatenate([rows[d], rows[d + 1]], axis=1) for d in range(3)], axis=0)
                got = jnp.dot(weight[...], tile, preferred_element_type=F32)
                for xo in range(2):
                    for yo in range(2):
                        g = got[yo * 3 * C:(yo + 1) * 3 * C, xo * Z:(xo + 1) * Z]
                        v = g[C:2 * C] + after(g[0:C]) + before(g[2 * C:])
                        write(i, j, xo, yo, v)
            return carry
        lax.fori_loop(0, width // 2, trip, 0)

    def mask_of(i, j, xo, yo, reach):
        bx = (2 * i + xo + 8 - reach) >> 3
        by = (2 * j + yo + 8 - reach) >> 3
        return mask[bx][by:by + 1, :]

    def cell(y):
        return slice(y * C, (y + 1) * C)

    def write_hidden(i, j, xo, yo, v):
        m = mask_of(i, j, xo, yo, H - 1)
        hid[2 * i + xo, cell(2 * j + yo), :] = (jnp.maximum(v + b1[...], 0.0) * m).astype(BF)

    def write_two(i, j, xo, yo, v):
        m = mask_of(i, j, xo, yo, H - 2)
        grad = ups[i, cell(j), 0:Z]
        pick = ups[i, cell(j), Z:2 * Z]
        live = (pick == odd + float(4 * xo + 2 * yo)) & (v + b2[...] > 0.0)
        two[2 * i + xo, cell(2 * j + yo), :] = jnp.where(live, grad * m, 0.0).astype(BF)

    def write_one(i, j, xo, yo, v):
        h = hid[2 * i + xo + 2, cell(2 * j + yo + 2), :].astype(F32)
        one[2 * i + xo, cell(2 * j + yo), :] = jnp.where(h > 0.0, v, 0.0).astype(BF)

    def write_out(i, j, xo, yo, v):
        m = mask_of(i, j, xo, yo, 0)
        out[2 * i + xo, cell(2 * j + yo), :] = (v * m).astype(BF)

    conv(feat, w1, W - 2, write_hidden)
    conv(hid, w2, W - 4, write_two)
    conv(two, f2, W - 6, write_one)
    conv(one, f1, W - 8, write_out)

    def weight_grad(src, off_s, delta, off_d, acc):
        def trip(x, sums):
            total, bias = sums
            lefts, rights = [], []
            for y in range(N):
                d = delta[x + off_d, cell(y + off_d), :].astype(F32)
                bias = bias + d
                rights.append(jnp.concatenate([before(d), d, after(d)], axis=0).astype(BF))
            right = jnp.concatenate(rights, axis=1)
            left = jnp.concatenate(
                [jnp.concatenate(
                    [src[x + off_s + a, (y + off_s) * C:(y + off_s + 3) * C, :] for y in range(N)],
                    axis=1) for a in range(3)], axis=0)
            got = lax.dot_general(left, right, (((1,), (1,)), ((), ())), preferred_element_type=F32)
            acc[...] += got
            return total, bias
        acc[...] = jnp.zeros_like(acc)
        _, bias = lax.fori_loop(0, N, trip, (0, jnp.zeros((C, Z), F32)))
        return jnp.broadcast_to(jnp.sum(bias, axis=1, keepdims=True), (C, Z))

    bias2 = weight_grad(hid, H - 2, two, H - 2, acc2)
    bias1 = weight_grad(feat, H - 1, one, H - 3, acc1)
    rows9 = 9 * C
    pad = jnp.zeros((rows9, Z - 3 * C), F32)
    parts[0:rows9, :] = jnp.concatenate([acc1[...], pad], axis=1).astype(BF)
    parts[rows9:2 * rows9, :] = jnp.concatenate([acc2[...], pad], axis=1).astype(BF)
    parts[2 * rows9:2 * rows9 + C, :] = bias1.astype(BF)
    parts[2 * rows9 + C:2 * rows9 + 2 * C, :] = bias2.astype(BF)


def body(features, occupancy, weight_one, bias_one, weight_two, bias_two, grad_pooled, pool_choice):
    C, nx, ny, Z = features.shape
    qx, qy = nx // 2, ny // 2
    H = HALO
    axes = ("gx", "gy")
    devices = lax.axis_size("gx") * lax.axis_size("gy")
    flags = jnp.pad(occupancy, ((1, 1), (1, 1), (0, 0)))
    window = lax.dynamic_slice(
        flags, (lax.axis_index("gx"), lax.axis_index("gy"), jnp.int32(0)), (3, 3, occupancy.shape[2]))
    mask = jnp.repeat(window, 8, axis=2).astype(F32)
    own = features.transpose(1, 2, 0, 3) * mask[1, 1].astype(BF)
    mask = jnp.pad(mask, ((0, 0), (0, 5), (0, 0)))
    pown = jnp.concatenate([grad_pooled, pool_choice.astype(BF)], axis=3).transpose(1, 2, 0, 3)

    def msg(cells, pooled):
        return jnp.concatenate([cells.reshape(-1, C, Z), pooled.reshape(-1, C, Z)], axis=0)

    xlow = shift(msg(own[nx - H:], pown[qx - 1:]), "gx", 1)
    xhigh = shift(msg(own[:H], pown[:1]), "gx", -1)

    def side(ys, qs):
        def pieces(m):
            return m[:H * ny].reshape(H, ny, C, Z)[:, ys], m[H * ny:].reshape(1, qy, C, Z)[:, qs]
        lc, lp = pieces(xlow)
        hc, hp = pieces(xhigh)
        return msg(jnp.concatenate([lc, own[:, ys], hc], axis=0),
                   jnp.concatenate([lp, pown[:, qs], hp], axis=0))

    ylow = shift(side(slice(ny - H, ny), slice(qy - 1, qy)), "gy", 1)
    yhigh = shift(side(slice(0, H), slice(0, 1)), "gy", -1)

    w = nx + 2 * H
    out, parts = pl.pallas_call(
        section,
        out_shape=(jax.ShapeDtypeStruct((nx, ny * C, Z), BF),
                   jax.ShapeDtypeStruct((20 * C, Z), BF)),
        scratch_shapes=[
            pltpu.VMEM((w, w * C, Z), BF),
            pltpu.VMEM((qx + 2, (qy + 2) * C, Z), BF),
            pltpu.VMEM((w - 2, (w - 2) * C, Z), BF),
            pltpu.VMEM((w - 4, (w - 4) * C, Z), BF),
            pltpu.VMEM((w - 6, (w - 6) * C, Z), BF),
            pltpu.VMEM((qx + 2, (qy + 2) * C, 2 * Z), F32),
            pltpu.VMEM((9 * C, 3 * C), F32),
            pltpu.VMEM((9 * C, 3 * C), F32),
        ],
        compiler_params=pltpu.CompilerParams(vmem_limit_bytes=40 << 20),
        name="section",
    )(own.reshape(nx, ny * C, Z), xlow, xhigh, ylow, yhigh, pown.reshape(qx, qy * C, Z), mask,
      toeplitz(weight_one), toeplitz(weight_two), toeplitz(flipped(weight_two)),
      toeplitz(flipped(weight_one)),
      jnp.broadcast_to(bias_one[:, None], (C, Z)), jnp.broadcast_to(bias_two[:, None], (C, Z)))

    rows = 20 * C // devices
    got = lax.all_to_all(parts.reshape(devices, rows, Z), axes, 0, 0, tiled=True)
    mine = jnp.sum(got.astype(F32), axis=0).astype(BF)
    spread = jnp.broadcast_to(mine[None], (devices, rows, Z))
    summed = lax.all_to_all(spread, axes, 0, 0, tiled=True).reshape(20 * C, Z).astype(F32)
    cells = nx * lax.axis_size("gx") * ny * lax.axis_size("gy") * Z
    summed = summed * (1.0 / math.sqrt(cells))

    def unpack(block):
        return block[:, :3 * C].reshape(3, 3, C, 3, C).transpose(4, 0, 1, 3, 2)

    grad_input = out.reshape(nx, ny, C, Z).transpose(2, 0, 1, 3)
    return (grad_input, unpack(summed[:9 * C]), summed[18 * C:19 * C, 0],
            unpack(summed[9 * C:18 * C]), summed[19 * C:, 0])


def solution(mesh):
    cell = P(None, "gx", "gy", None)
    return jax.shard_map(
        body,
        mesh=mesh,
        in_specs=(cell, P(), P(), P(), P(), P(), cell, cell),
        out_specs=(cell, P(), P(), P(), P()),
        check_vma=False,
    )
```

```python
import math

import jax
import jax.numpy as jnp
from jax import lax
from jax.experimental import pallas as pl
from jax.experimental.pallas import tpu as pltpu
from jax.sharding import PartitionSpec as P

BF = jnp.bfloat16
F32 = jnp.float32
C, Z, N, H = 32, 128, 8, 4
W = N + 2 * H
Q = N // 2
ROWS = 8


def call(kernel, outs, scratch=(), name=None):
    return pl.pallas_call(
        kernel,
        out_shape=tuple(jax.ShapeDtypeStruct(s, d) for s, d in outs),
        scratch_shapes=[pltpu.VMEM(s, d) for s, d in scratch],
        compiler_params=pltpu.CompilerParams(vmem_limit_bytes=40 << 20),
        name=name,
    )


def shift(v, axis, step):
    devices = lax.axis_size(axis)
    pairs = [(i, i + step) for i in range(devices) if 0 <= i + step < devices]
    return lax.ppermute(v, axis, pairs)


def cell(y, n=1):
    return slice(y * C, (y + n) * C)


def prepare(w1, w2, b1, b2, t1, t2, f2, f1, c1, c2):
    zero = jnp.zeros((C, C), F32)
    for src, plain, flip in ((w1, t1, f1), (w2, t2, f2)):
        for a in range(3):
            for c in range(3):
                rows = slice(c * C, (c + 1) * C)
                high = slice((3 + c) * C, (4 + c) * C)
                cols = slice(a * 4 * C, (a + 1) * 4 * C)
                line = jnp.concatenate(
                    [src[a * 9 + b * 3 + c].astype(F32) for b in range(3)] + [zero], axis=1)
                plain[rows, cols] = line.astype(BF)
                plain[high, cols] = pltpu.roll(line, C, 1).astype(BF)
                tall = jnp.concatenate(
                    [src[(2 - a) * 9 + (2 - b) * 3 + 2 - c].astype(F32) for b in range(3)] + [zero],
                    axis=0)
                line = jnp.transpose(tall)
                flip[rows, cols] = line.astype(BF)
                flip[high, cols] = pltpu.roll(line, C, 1).astype(BF)
    for src, dst in ((b1, c1), (b2, c2)):
        dst[...] = jnp.transpose(jnp.broadcast_to(src[...], (Z, C)))


def pack_y(own, pown, mlow, mhigh):
    for x in range(N):
        for k in range(H):
            mlow[x * H + k] = own[x, cell(N - H + k), :]
            mhigh[x * H + k] = own[x, cell(k), :]
    for x in range(Q):
        mlow[N * H + x] = pown[x, cell(Q - 1), :]
        mhigh[N * H + x] = pown[x, cell(0), :]


def pack_x(own, pown, ylow, yhigh, feat, pool, mlow, mhigh):
    for x in range(N):
        feat[x, cell(H, N), :] = own[x]
        for k in range(H):
            feat[x, cell(k), :] = ylow[x * H + k]
            feat[x, cell(H + N + k), :] = yhigh[x * H + k]
    for x in range(Q):
        pool[x, cell(1, Q), :] = pown[x]
        pool[x, cell(0), :] = ylow[N * H + x]
        pool[x, cell(Q + 1), :] = yhigh[N * H + x]
    for k in range(H):
        for y in range(W):
            mlow[k * W + y] = feat[N - H + k, cell(y), :]
            mhigh[k * W + y] = feat[k, cell(y), :]
    for y in range(Q + 2):
        mlow[H * W + y] = pool[Q - 1, cell(y), :]
        mhigh[H * W + y] = pool[0, cell(y), :]


def after(v):
    lane = lax.broadcasted_iota(jnp.int32, v.shape, 1)
    return jnp.where(lane == 0, 0.0, pltpu.roll(v, 1, 1))


def before(v):
    lane = lax.broadcasted_iota(jnp.int32, v.shape, 1)
    return jnp.where(lane == Z - 1, 0.0, pltpu.roll(v, Z - 1, 1))


def spreader():
    row = lax.broadcasted_iota(jnp.int32, (Z, 2 * Z), 0)
    col = lax.broadcasted_iota(jnp.int32, (Z, 2 * Z), 1)
    return jnp.where(row == col // 2, 1.0, 0.0).astype(BF)


def conv_pair(src, x, weight, width, write, i):
    for j in range(width // 2):
        rows = [src[x + d, cell(2 * j, 4), :] for d in range(4)]
        tile = jnp.concatenate(
            [jnp.concatenate([rows[d], rows[d + 1]], axis=1) for d in range(3)], axis=0)
        got = jnp.dot(weight[...], tile, preferred_element_type=F32)
        for xo in range(2):
            for yo in range(2):
                g = got[yo * 3 * C:(yo + 1) * 3 * C, xo * Z:(xo + 1) * Z]
                v = g[C:2 * C] + after(g[0:C]) + before(g[2 * C:])
                write(i, j, xo, yo, v)


def writers(mask, b1, b2, ups, hid, two, one, at):
    lane = lax.broadcasted_iota(jnp.int32, (C, Z), 1)
    odd = (lane % 2).astype(F32)

    def mask_of(i, j, xo, yo, reach):
        bx = (2 * i + xo + N - reach) >> 3
        by = (2 * j + yo + N - reach) >> 3
        return mask[bx][by:by + 1, :]

    def write_hidden(i, j, xo, yo, v):
        m = mask_of(i, j, xo, yo, H - 1)
        hid[2 * i + xo - at[0], cell(2 * j + yo), :] = (
            jnp.maximum(v + b1[...], 0.0) * m).astype(BF)

    def write_two(i, j, xo, yo, v):
        m = mask_of(i, j, xo, yo, H - 2)
        grad = ups[i - at[3], cell(j), 0:Z]
        pick = ups[i - at[3], cell(j), Z:2 * Z]
        live = (pick == odd + float(4 * xo + 2 * yo)) & (v + b2[...] > 0.0)
        two[2 * i + xo - at[1], cell(2 * j + yo), :] = jnp.where(live, grad * m, 0.0).astype(BF)

    def write_one(i, j, xo, yo, v):
        h = hid[2 * i + xo + 2 - at[0], cell(2 * j + yo + 2), :].astype(F32)
        one[2 * i + xo - at[2], cell(2 * j + yo), :] = jnp.where(h > 0.0, v, 0.0).astype(BF)

    return write_hidden, write_two, write_one


def middle(feat, pool, mask, t1, t2, f2, b1, b2, hid, two, one, ups):
    spread = spreader()
    for p in range(2):
        ups[p] = jnp.dot(pool[1 + p], spread, preferred_element_type=F32)
    write_hidden, write_two, write_one = writers(mask, b1, b2, ups, hid, two, one, (4, 4, 4, 2))

    def trip(t, carry):
        conv_pair(feat, 2 * t, t1, W - 2, write_hidden, t + 2)
        return carry
    lax.fori_loop(0, 3, trip, 0)
    for i in (2, 3):
        conv_pair(hid, 2 * i - 4, t2, W - 4, write_two, i)
    conv_pair(two, 0, f2, W - 6, write_one, 2)


def outer(mfeat, mpool, xlow, xhigh, mhid, mtwo, mone, mask, t1, t2, f2, b1, b2,
          one, parts, feat, hid, two, ups, acc1, acc2):
    for x in range(N):
        feat[H + x] = mfeat[x]
    for k in range(H):
        for y in range(W):
            feat[k, cell(y), :] = xlow[k * W + y]
            feat[H + N + k, cell(y), :] = xhigh[k * W + y]
    for x in range(6):
        hid[4 + x] = mhid[x]
    for x in range(4):
        two[4 + x] = mtwo[x]
    for x in range(2):
        one[4 + x] = mone[x]
    spread = spreader()
    for y in range(Q + 2):
        ups[0, cell(y), :] = jnp.dot(xlow[H * W + y], spread, preferred_element_type=F32)
        ups[Q + 1, cell(y), :] = jnp.dot(xhigh[H * W + y], spread, preferred_element_type=F32)
    ups[1] = jnp.dot(mpool[0], spread, preferred_element_type=F32)
    ups[Q] = jnp.dot(mpool[Q - 1], spread, preferred_element_type=F32)
    write_hidden, write_two, write_one = writers(mask, b1, b2, ups, hid, two, one, (0, 0, 0, 0))

    def rim(src, weight, width, write):
        half = width // 2

        def trip(t, carry):
            for k in range(2):
                i = t * (half - 2) + k
                conv_pair(src, 2 * i, weight, width, write, i)
            return carry
        lax.fori_loop(0, 2, trip, 0)

    rim(feat, t1, W - 2, write_hidden)
    rim(hid, t2, W - 4, write_two)
    rim(two, f2, W - 6, write_one)

    def term(x, bias, src, off_s, delta, off_d, acc):
        rights = []
        for y in range(N):
            d = delta[x + off_d, cell(y + off_d), :].astype(F32)
            bias = bias + d
            rights.append(jnp.concatenate([before(d), d, after(d)], axis=0).astype(BF))
        left = jnp.concatenate(
            [jnp.concatenate([src[x + off_s + a, cell(y + off_s, 3), :] for y in range(N)], axis=1)
             for a in range(3)], axis=0)
        acc[...] += lax.dot_general(left, jnp.concatenate(rights, axis=1), (((1,), (1,)), ((), ())),
                                    preferred_element_type=F32)
        return bias

    def trip(x, sums):
        s2 = term(x, sums[1], hid, H - 2, two, H - 2, acc2)
        s1 = term(x, sums[0], feat, H - 1, one, H - 3, acc1)
        return s1, s2

    acc1[...] = jnp.zeros_like(acc1)
    acc2[...] = jnp.zeros_like(acc2)
    none = jnp.zeros((C, Z), F32)
    sums = lax.fori_loop(0, N, trip, (none, none))
    rows9 = 9 * C
    pad = jnp.zeros((rows9, Z - 3 * C), F32)
    for k, acc in enumerate((acc1, acc2)):
        parts[k * rows9:(k + 1) * rows9, :] = jnp.concatenate([acc[...], pad], axis=1).astype(BF)
        total = jnp.sum(sums[k], axis=1, keepdims=True)
        parts[2 * rows9 + k * C:2 * rows9 + (k + 1) * C, :] = jnp.broadcast_to(
            total, (C, Z)).astype(BF)
    rest = parts.shape[0] - 20 * C
    parts[20 * C:, :] = jnp.zeros((rest, Z), BF)


def final(one, mask, f1, out):
    def write_out(i, j, xo, yo, v):
        out[2 * i + xo, cell(2 * j + yo), :] = (v * mask[1][1:2, :]).astype(BF)

    def trip(t, carry):
        for k in range(2):
            conv_pair(one, 4 * t + 2 * k, f1, N, write_out, 2 * t + k)
        return carry
    lax.fori_loop(0, N // 4, trip, 0)


def body(features, occupancy, weight_one, bias_one, weight_two, bias_two, grad_pooled, pool_choice):
    axes = ("gx", "gy")
    devices = lax.axis_size("gx") * lax.axis_size("gy")
    flags = jnp.pad(occupancy, ((1, 1), (1, 1), (0, 0)))
    window = lax.dynamic_slice(
        flags, (lax.axis_index("gx"), lax.axis_index("gy"), jnp.int32(0)), (3, 3, occupancy.shape[2]))
    mask = jnp.repeat(window, 8, axis=2).astype(F32)
    own = (features * mask[1, 1].astype(BF)).transpose(1, 2, 0, 3).reshape(N, N * C, Z)
    mask = jnp.pad(mask, ((0, 0), (0, 5), (0, 0)))
    pown = jnp.concatenate([grad_pooled, pool_choice.astype(BF)], axis=3)
    pown = pown.transpose(1, 2, 0, 3).reshape(Q, Q * C, Z)

    ymsg = N * H + Q
    mlow, mhigh = call(pack_y, [((ymsg, C, Z), BF)] * 2, name="pack_y")(own, pown)
    ylow = shift(mlow, "gy", 1)
    yhigh = shift(mhigh, "gy", -1)

    def blocks(weight):
        return weight.transpose(1, 2, 3, 0, 4).reshape(27, C, C)

    t1, t2, f2, f1, b1, b2 = call(
        prepare, [((6 * C, 12 * C), BF)] * 4 + [((C, Z), F32)] * 2, name="prepare")(
            blocks(weight_one), blocks(weight_two), bias_one.reshape(1, C), bias_two.reshape(1, C))

    own, pown, t1 = lax.optimization_barrier((own, pown, t1))
    xmsg = W * H + Q + 2
    mfeat, mpool, mlow, mhigh = call(
        pack_x, [((N, W * C, Z), BF), ((Q, (Q + 2) * C, Z), BF)] + [((xmsg, C, Z), BF)] * 2,
        name="pack_x")(own, pown, ylow, yhigh)
    xlow = shift(mlow, "gx", 1)
    xhigh = shift(mhigh, "gx", -1)

    mhid, mtwo, mone = call(
        middle,
        [((6, (W - 2) * C, Z), BF), ((4, (W - 4) * C, Z), BF), ((2, (W - 6) * C, Z), BF)],
        [((2, (Q + 2) * C, 2 * Z), F32)], name="middle")(mfeat, mpool, mask, t1, t2, f2, b1, b2)

    one, parts = call(
        outer, [((W - 6, (W - 6) * C, Z), BF), ((devices * ROWS, Z), BF)],
        [((W, W * C, Z), BF), ((W - 2, (W - 2) * C, Z), BF), ((W - 4, (W - 4) * C, Z), BF),
         ((Q + 2, (Q + 2) * C, 2 * Z), F32), ((9 * C, 3 * C), F32), ((9 * C, 3 * C), F32)],
        name="outer")(mfeat, mpool, xlow, xhigh, mhid, mtwo, mone, mask, t1, t2, f2, b1, b2)

    got = lax.all_to_all(parts.reshape(devices, ROWS, Z), axes, 0, 0, tiled=True)
    out, = call(final, [((N, N * C, Z), BF)], name="final")(one, mask, f1)
    mine = jnp.sum(got.astype(F32), axis=0).astype(BF)
    spread = jnp.broadcast_to(mine[None], (devices, ROWS, Z))
    summed = lax.all_to_all(spread, axes, 0, 0, tiled=True).reshape(devices * ROWS, Z).astype(F32)
    cells = N * lax.axis_size("gx") * N * lax.axis_size("gy") * Z
    summed = summed * (1.0 / math.sqrt(cells))

    def unpack(block):
        return block[:, :3 * C].reshape(3, 3, C, 3, C).transpose(4, 0, 1, 3, 2)

    grad_input = out.reshape(N, N, C, Z).transpose(2, 0, 1, 3)
    return (grad_input, unpack(summed[:9 * C]), summed[18 * C:19 * C, 0],
            unpack(summed[9 * C:18 * C]), summed[19 * C:20 * C, 0])


def solution(mesh):
    cells = P(None, "gx", "gy", None)
    return jax.shard_map(
        body,
        mesh=mesh,
        in_specs=(cells, P(), P(), P(), P(), P(), cells, cells),
        out_specs=(cells, P(), P(), P(), P()),
        check_vma=False,
    )
```

```python
import math

import jax
import jax.numpy as jnp
from jax import lax
from jax.experimental import pallas as pl
from jax.experimental.pallas import tpu as pltpu
from jax.sharding import PartitionSpec as P

BF = jnp.bfloat16
F32 = jnp.float32
C, Z, N, H = 32, 128, 8, 4
W = N + 2 * H
Q = N // 2
ROWS = 8
CELLS = 128 * 64 * 128


def call(kernel, outs, scratch=(), name=None):
    return pl.pallas_call(
        kernel,
        out_shape=tuple(jax.ShapeDtypeStruct(s, d) for s, d in outs),
        scratch_shapes=[pltpu.VMEM(s, d) for s, d in scratch],
        compiler_params=pltpu.CompilerParams(vmem_limit_bytes=40 << 20),
        name=name,
    )


def shift(v, axis, step):
    devices = lax.axis_size(axis)
    pairs = [(i, i + step) for i in range(devices) if 0 <= i + step < devices]
    return lax.ppermute(v, axis, pairs)


def cell(y, n=1):
    return slice(y * C, (y + n) * C)


def prepare(w1, w2, b1, b2, t1, t2, f2, f1, c1, c2):
    zero = jnp.zeros((C, C), F32)
    for src, plain, flip in ((w1, t1, f1), (w2, t2, f2)):
        for a in range(3):
            for c in range(3):
                rows = slice(c * C, (c + 1) * C)
                high = slice((3 + c) * C, (4 + c) * C)
                cols = slice(a * 4 * C, (a + 1) * 4 * C)
                line = jnp.concatenate(
                    [src[a * 9 + b * 3 + c].astype(F32) for b in range(3)] + [zero], axis=1)
                plain[rows, cols] = line.astype(BF)
                plain[high, cols] = pltpu.roll(line, C, 1).astype(BF)
                tall = jnp.concatenate(
                    [src[(2 - a) * 9 + (2 - b) * 3 + 2 - c].astype(F32) for b in range(3)] + [zero],
                    axis=0)
                line = jnp.transpose(tall)
                flip[rows, cols] = line.astype(BF)
                flip[high, cols] = pltpu.roll(line, C, 1).astype(BF)
    for src, dst in ((b1, c1), (b2, c2)):
        dst[...] = jnp.transpose(jnp.broadcast_to(src[...], (Z, C)))


def pack_y(own, pown, mlow, mhigh):
    for x in range(N):
        for k in range(H):
            mlow[x * H + k] = own[x, cell(N - H + k), :]
            mhigh[x * H + k] = own[x, cell(k), :]
    for x in range(Q):
        mlow[N * H + x] = pown[x, cell(Q - 1), :]
        mhigh[N * H + x] = pown[x, cell(0), :]


def pack_x(own, pown, ylow, yhigh, feat, pool, mlow, mhigh):
    for x in range(N):
        feat[x, cell(H, N), :] = own[x]
        for k in range(H):
            feat[x, cell(k), :] = ylow[x * H + k]
            feat[x, cell(H + N + k), :] = yhigh[x * H + k]
    for x in range(Q):
        pool[x, cell(1, Q), :] = pown[x]
        pool[x, cell(0), :] = ylow[N * H + x]
        pool[x, cell(Q + 1), :] = yhigh[N * H + x]
    for k in range(H):
        for y in range(W):
            mlow[k * W + y] = feat[N - H + k, cell(y), :]
            mhigh[k * W + y] = feat[k, cell(y), :]
    for y in range(Q + 2):
        mlow[H * W + y] = pool[Q - 1, cell(y), :]
        mhigh[H * W + y] = pool[0, cell(y), :]


def after(v):
    lane = lax.broadcasted_iota(jnp.int32, v.shape, 1)
    return jnp.where(lane == 0, 0.0, pltpu.roll(v, 1, 1))


def before(v):
    lane = lax.broadcasted_iota(jnp.int32, v.shape, 1)
    return jnp.where(lane == Z - 1, 0.0, pltpu.roll(v, Z - 1, 1))


def spreader():
    row = lax.broadcasted_iota(jnp.int32, (Z, 2 * Z), 0)
    col = lax.broadcasted_iota(jnp.int32, (Z, 2 * Z), 1)
    return jnp.where(row == col // 2, 1.0, 0.0).astype(BF)


def conv_pair(rows_at, x, weight, width, write, i):
    for j in range(width // 2):
        rows = [rows_at(x + d, 2 * j, 4) for d in range(4)]
        tile = jnp.concatenate(
            [jnp.concatenate([rows[d], rows[d + 1]], axis=1) for d in range(3)], axis=0)
        got = jnp.dot(weight[...], tile, preferred_element_type=F32)
        for xo in range(2):
            for yo in range(2):
                g = got[yo * 3 * C:(yo + 1) * 3 * C, xo * Z:(xo + 1) * Z]
                v = g[C:2 * C] + after(g[0:C]) + before(g[2 * C:])
                write(i, j, xo, yo, v)


def planes(ref, first=0):
    def rows_at(x, y, n=1):
        return ref[x - first, cell(y, n), :]
    return rows_at


def writers(mask, b1, b2, ups_at, hid_at, hid_put, two_put, one_put):
    lane = lax.broadcasted_iota(jnp.int32, (C, Z), 1)
    odd = (lane % 2).astype(F32)

    def mask_of(i, j, xo, yo, reach):
        bx = (2 * i + xo + N - reach) >> 3
        by = (2 * j + yo + N - reach) >> 3
        return mask[bx][by:by + 1, :]

    def write_hidden(i, j, xo, yo, v):
        m = mask_of(i, j, xo, yo, H - 1)
        hid_put(2 * i + xo, 2 * j + yo, (jnp.maximum(v + b1[...], 0.0) * m).astype(BF))

    def write_two(i, j, xo, yo, v):
        m = mask_of(i, j, xo, yo, H - 2)
        grad, pick = ups_at(i, j)
        live = (pick == odd + float(4 * xo + 2 * yo)) & (v + b2[...] > 0.0)
        two_put(2 * i + xo, 2 * j + yo, jnp.where(live, grad * m, 0.0).astype(BF))

    def write_one(i, j, xo, yo, v):
        h = hid_at(2 * i + xo + 2, 2 * j + yo + 2).astype(F32)
        one_put(2 * i + xo, 2 * j + yo, jnp.where(h > 0.0, v, 0.0).astype(BF))

    return write_hidden, write_two, write_one


def putter(ref, index):
    def put(x, y, v):
        ref[index(x), cell(y), :] = v
    return put


def upstream(ups, index):
    def ups_at(i, j):
        return ups[index(i), cell(j), 0:Z], ups[index(i), cell(j), Z:2 * Z]
    return ups_at


def term(x, bias, src_at, off_s, delta_at, off_d, acc):
    rights = []
    for y in range(N):
        d = delta_at(x + off_d, y + off_d).astype(F32)
        bias[...] += d
        rights.append(jnp.concatenate([before(d), d, after(d)], axis=0).astype(BF))
    left = jnp.concatenate(
        [jnp.concatenate([src_at(x + off_s + a, y + off_s, 3) for y in range(N)], axis=1)
         for a in range(3)], axis=0)
    acc[...] += lax.dot_general(left, jnp.concatenate(rights, axis=1), (((1,), (1,)), ((), ())),
                                preferred_element_type=F32)


def middle(feat, pool, mask, t1, t2, f2, b1, b2, hid, two, one, acc1, acc2, s1, s2, ups):
    spread = spreader()
    for p in range(2):
        ups[p] = jnp.dot(pool[1 + p], spread, preferred_element_type=F32)
    feat_at, hid_at, two_at, one_at = planes(feat, 4), planes(hid, 4), planes(two, 4), planes(one, 4)
    mid = lambda x: x - 4
    write_hidden, write_two, write_one = writers(
        mask, b1, b2, upstream(ups, lambda i: i - 2), hid_at,
        putter(hid, mid), putter(two, mid), putter(one, mid))
    for ref in (acc1, acc2, s1, s2):
        ref[...] = jnp.zeros_like(ref)
    for i in (2, 3, 4):
        conv_pair(feat_at, 2 * i, t1, W - 2, write_hidden, i)
    for i in (2, 3):
        conv_pair(hid_at, 2 * i, t2, W - 4, write_two, i)
    conv_pair(two_at, 4, f2, W - 6, write_one, 2)
    for x in range(2, 6):
        term(x, s2, hid_at, H - 2, two_at, H - 2, acc2)
    for x in range(3, 5):
        term(x, s1, feat_at, H - 1, one_at, H - 3, acc1)


def outer(mfeat, mpool, xlow, xhigh, mhid, mtwo, mone, macc1, macc2, ms1, ms2, mask,
          t1, t2, f2, b1, b2, one, parts, hid, two, ups, acc1, acc2, s1, s2):
    def feat_at(x, y, n=1):
        if H <= x < H + N:
            return mfeat[x - H, cell(y, n), :]
        ref, k = (xlow, x) if x < H else (xhigh, x - H - N)
        return ref[k * W + y:k * W + y + n].reshape(n * C, Z)

    spread = spreader()
    for y in range(Q + 2):
        ups[0, cell(y), :] = jnp.dot(xlow[H * W + y], spread, preferred_element_type=F32)
        ups[3, cell(y), :] = jnp.dot(xhigh[H * W + y], spread, preferred_element_type=F32)
    ups[1] = jnp.dot(mpool[0], spread, preferred_element_type=F32)
    ups[2] = jnp.dot(mpool[Q - 1], spread, preferred_element_type=F32)

    def merged(ref, mid, count):
        def rows_at(x, y, n=1):
            if 4 <= x < 4 + count:
                return mid[x - 4, cell(y, n), :]
            return ref[x if x < 4 else x - count, cell(y, n), :]
        return rows_at

    hid_at, two_at = merged(hid, mhid, 6), merged(two, mtwo, 4)
    one_at = planes(one)
    for x in range(2):
        one[4 + x] = mone[x]
    write_hidden, write_two, write_one = writers(
        mask, b1, b2, upstream(ups, lambda i: i if i < 2 else i - 2), hid_at,
        putter(hid, lambda x: x if x < 4 else x - 6),
        putter(two, lambda x: x if x < 4 else x - 4), putter(one, lambda x: x))
    acc1[...] = macc1[...]
    acc2[...] = macc2[...]
    s1[...] = ms1[...]
    s2[...] = ms2[...]
    for i in (0, 1, 5, 6):
        conv_pair(feat_at, 2 * i, t1, W - 2, write_hidden, i)
    for i in (0, 1, 4, 5):
        conv_pair(hid_at, 2 * i, t2, W - 4, write_two, i)
    for i in (0, 1, 3, 4):
        conv_pair(two_at, 2 * i, f2, W - 6, write_one, i)
    for x in (0, 1, 6, 7):
        term(x, s2, hid_at, H - 2, two_at, H - 2, acc2)
    for x in (0, 1, 2, 5, 6, 7):
        term(x, s1, feat_at, H - 1, one_at, H - 3, acc1)
    rows9 = 9 * C
    pad = jnp.zeros((rows9, Z - 3 * C), F32)
    for k, (acc, sums) in enumerate(((acc1, s1), (acc2, s2))):
        parts[k * rows9:(k + 1) * rows9, :] = jnp.concatenate([acc[...], pad], axis=1).astype(BF)
        total = jnp.sum(sums[...], axis=1, keepdims=True)
        parts[2 * rows9 + k * C:2 * rows9 + (k + 1) * C, :] = jnp.broadcast_to(
            total, (C, Z)).astype(BF)
    rest = parts.shape[0] - 20 * C
    parts[20 * C:, :] = jnp.zeros((rest, Z), BF)


def add_up(got, out):
    total = jnp.sum(got[...].astype(F32), axis=0, keepdims=True).astype(BF)
    out[...] = jnp.broadcast_to(total, out.shape)


def unpack(summed, w1, w2, b1, b2):
    scale = 1.0 / math.sqrt(CELLS)
    rows9 = 9 * C
    for k, (w, b) in enumerate(((w1, b1), (w2, b2))):
        for n in range(9):
            rows = slice(k * rows9 + n * C, k * rows9 + (n + 1) * C)
            block = jnp.transpose(summed[rows, :].astype(F32) * scale)
            for c in range(3):
                w[n * 3 + c] = block[c * C:(c + 1) * C, :]
        rows = slice(2 * rows9 + k * C, 2 * rows9 + (k + 1) * C)
        b[...] = jnp.transpose(summed[rows, :].astype(F32) * scale)[0:1, :]


def final(one, mask, f1, out):
    def write_out(i, j, xo, yo, v):
        out[2 * i + xo, cell(2 * j + yo), :] = (v * mask[1][1:2, :]).astype(BF)

    for i in range(N // 2):
        conv_pair(planes(one), 2 * i, f1, N, write_out, i)


def body(features, occupancy, weight_one, bias_one, weight_two, bias_two, grad_pooled, pool_choice):
    axes = ("gx", "gy")
    devices = lax.axis_size("gx") * lax.axis_size("gy")
    flags = jnp.pad(occupancy, ((1, 1), (1, 1), (0, 0)))
    window = lax.dynamic_slice(
        flags, (lax.axis_index("gx"), lax.axis_index("gy"), jnp.int32(0)), (3, 3, occupancy.shape[2]))
    mask = jnp.repeat(window, 8, axis=2).astype(F32)
    own = (features * mask[1, 1].astype(BF)).transpose(1, 2, 0, 3).reshape(N, N * C, Z)
    mask = jnp.pad(mask, ((0, 0), (0, 5), (0, 0)))
    pown = jnp.concatenate([grad_pooled, pool_choice.astype(BF)], axis=3)
    pown = pown.transpose(1, 2, 0, 3).reshape(Q, Q * C, Z)

    ymsg = N * H + Q
    mlow, mhigh = call(pack_y, [((ymsg, C, Z), BF)] * 2, name="pack_y")(own, pown)
    ylow = shift(mlow, "gy", 1)
    yhigh = shift(mhigh, "gy", -1)

    def blocks(weight):
        return weight.transpose(1, 2, 3, 0, 4).reshape(27, C, C)

    t1, t2, f2, f1, b1, b2 = call(
        prepare, [((6 * C, 12 * C), BF)] * 4 + [((C, Z), F32)] * 2, name="prepare")(
            blocks(weight_one), blocks(weight_two), bias_one.reshape(1, C), bias_two.reshape(1, C))

    own, pown, t1 = lax.optimization_barrier((own, pown, t1))
    xmsg = W * H + Q + 2
    mfeat, mpool, mlow, mhigh = call(
        pack_x, [((N, W * C, Z), BF), ((Q, (Q + 2) * C, Z), BF)] + [((xmsg, C, Z), BF)] * 2,
        name="pack_x")(own, pown, ylow, yhigh)
    xlow = shift(mlow, "gx", 1)
    xhigh = shift(mhigh, "gx", -1)

    grads = [((9 * C, 3 * C), F32)] * 2 + [((C, Z), F32)] * 2
    mids = call(
        middle,
        [((6, (W - 2) * C, Z), BF), ((4, (W - 4) * C, Z), BF), ((2, (W - 6) * C, Z), BF)] + grads,
        [((2, (Q + 2) * C, 2 * Z), F32)], name="middle")(mfeat, mpool, mask, t1, t2, f2, b1, b2)

    one, parts = call(
        outer, [((W - 6, (W - 6) * C, Z), BF), ((devices * ROWS, Z), BF)],
        [((8, (W - 2) * C, Z), BF), ((8, (W - 4) * C, Z), BF),
         ((4, (Q + 2) * C, 2 * Z), F32)] + grads,
        name="outer")(mfeat, mpool, xlow, xhigh, *mids, mask, t1, t2, f2, b1, b2)

    block = (devices, ROWS, Z)
    got = lax.all_to_all(parts.reshape(block), axes, 0, 0, tiled=True)
    out, = call(final, [((N, N * C, Z), BF)], name="final")(one, mask, f1)
    mine, = call(add_up, [(block, BF)], name="add_up")(got)
    summed = lax.all_to_all(mine, axes, 0, 0, tiled=True).reshape(devices * ROWS, Z)
    gw1, gw2, gb1, gb2 = call(
        unpack, [((27, C, C), F32)] * 2 + [((1, C), F32)] * 2, name="unpack")(summed)

    def weights(g):
        return g.reshape(3, 3, 3, C, C).transpose(3, 0, 1, 2, 4)

    grad_input = out.reshape(N, N, C, Z).transpose(2, 0, 1, 3)
    return grad_input, weights(gw1), gb1.reshape(C), weights(gw2), gb2.reshape(C)


def solution(mesh):
    cells = P(None, "gx", "gy", None)
    return jax.shard_map(
        body,
        mesh=mesh,
        in_specs=(cells, P(), P(), P(), P(), P(), cells, cells),
        out_specs=(cells, P(), P(), P(), P()),
        check_vma=False,
    )
```

```python
import math

import jax
import jax.numpy as jnp
from jax import lax
from jax.experimental import pallas as pl
from jax.experimental.pallas import tpu as pltpu
from jax.sharding import PartitionSpec as P


BF = jnp.bfloat16
F32 = jnp.float32
C, Z, N, H = 32, 128, 8, 4
W = N + 2 * H
Q = N // 2
ROWS = 8
CELLS = 128 * 64 * 128


def call(kernel, outs, scratch=()):
    return pl.pallas_call(
        kernel,
        out_shape=tuple(jax.ShapeDtypeStruct(s, d) for s, d in outs),
        scratch_shapes=[pltpu.VMEM(s, d) for s, d in scratch],
        compiler_params=pltpu.CompilerParams(vmem_limit_bytes=40 << 20),
    )


def shift(v, axis, step):
    devices = lax.axis_size(axis)
    pairs = [(i, i + step) for i in range(devices) if 0 <= i + step < devices]
    return lax.ppermute(v, axis, pairs)


def cell(y, n=1):
    return slice(y * C, (y + n) * C)


def prepare(w1, w2, b1, b2, t1, t2, f2, f1, c1, c2):
    zero = jnp.zeros((C, C), F32)
    for src, plain, flip in ((w1, t1, f1), (w2, t2, f2)):
        for a in range(3):
            for c in range(3):
                rows = slice(c * C, (c + 1) * C)
                high = slice((3 + c) * C, (4 + c) * C)
                cols = slice(a * 4 * C, (a + 1) * 4 * C)
                line = jnp.concatenate(
                    [src[a * 9 + b * 3 + c].astype(F32) for b in range(3)] + [zero], axis=1)
                plain[rows, cols] = line.astype(BF)
                plain[high, cols] = pltpu.roll(line, C, 1).astype(BF)
                tall = jnp.concatenate(
                    [src[(2 - a) * 9 + (2 - b) * 3 + 2 - c].astype(F32) for b in range(3)] + [zero],
                    axis=0)
                line = jnp.transpose(tall)
                flip[rows, cols] = line.astype(BF)
                flip[high, cols] = pltpu.roll(line, C, 1).astype(BF)
    for src, dst in ((b1, c1), (b2, c2)):
        dst[...] = jnp.transpose(jnp.broadcast_to(src[...], (Z, C)))


def pack_faces(own, pown, ylow, yhigh, xlow, xhigh):
    for x in range(N):
        for k in range(H):
            ylow[x * H + k] = own[x, cell(N - H + k), :]
            yhigh[x * H + k] = own[x, cell(k), :]
    for k in range(H):
        for y in range(N):
            xlow[k * N + y] = own[N - H + k, cell(y), :]
            xhigh[k * N + y] = own[k, cell(y), :]
    for q in range(Q):
        ylow[N * H + q] = pown[q, cell(Q - 1), :]
        yhigh[N * H + q] = pown[q, cell(0), :]
        xlow[N * H + q] = pown[Q - 1, cell(q), :]
        xhigh[N * H + q] = pown[0, cell(q), :]


def pack_corners(own, pown, ylow, yhigh, feat, pool, clow, chigh):
    for x in range(N):
        feat[x, cell(H, N), :] = own[x]
        for k in range(H):
            feat[x, cell(k), :] = ylow[x * H + k]
            feat[x, cell(H + N + k), :] = yhigh[x * H + k]
    for x in range(Q):
        pool[x, cell(1, Q), :] = pown[x]
        pool[x, cell(0), :] = ylow[N * H + x]
        pool[x, cell(Q + 1), :] = yhigh[N * H + x]
    for x in range(H):
        for k in range(H):
            clow[x * N + k] = ylow[(N - H + x) * H + k]
            clow[x * N + H + k] = yhigh[(N - H + x) * H + k]
            chigh[x * N + k] = ylow[x * H + k]
            chigh[x * N + H + k] = yhigh[x * H + k]
    clow[N * H] = ylow[N * H + Q - 1]
    clow[N * H + 1] = yhigh[N * H + Q - 1]
    chigh[N * H] = ylow[N * H]
    chigh[N * H + 1] = yhigh[N * H]


def after(v):
    lane = lax.broadcasted_iota(jnp.int32, v.shape, 1)
    return jnp.where(lane == 0, 0.0, pltpu.roll(v, 1, 1))


def before(v):
    lane = lax.broadcasted_iota(jnp.int32, v.shape, 1)
    return jnp.where(lane == Z - 1, 0.0, pltpu.roll(v, Z - 1, 1))


def spreader():
    row = lax.broadcasted_iota(jnp.int32, (Z, 2 * Z), 0)
    col = lax.broadcasted_iota(jnp.int32, (Z, 2 * Z), 1)
    return jnp.where(row == col // 2, 1.0, 0.0).astype(BF)


def conv_pair(rows_at, x, weight, width, write, i):
    for j in range(width // 2):
        rows = [rows_at(x + d, 2 * j, 4) for d in range(4)]
        tile = jnp.concatenate(
            [jnp.concatenate([rows[d], rows[d + 1]], axis=1) for d in range(3)], axis=0)
        got = jnp.dot(weight[...], tile, preferred_element_type=F32)
        for xo in range(2):
            for yo in range(2):
                g = got[yo * 3 * C:(yo + 1) * 3 * C, xo * Z:(xo + 1) * Z]
                v = g[C:2 * C] + after(g[0:C]) + before(g[2 * C:])
                write(i, j, xo, yo, v)


def planes(ref, first=0):
    def rows_at(x, y, n=1):
        return ref[x - first, cell(y, n), :]

    return rows_at


def writers(mask, b1, b2, ups_at, hid_at, hid_put, two_put, one_put):
    lane = lax.broadcasted_iota(jnp.int32, (C, Z), 1)
    odd = (lane % 2).astype(F32)

    def mask_of(i, j, xo, yo, reach):
        bx = (2 * i + xo + N - reach) >> 3
        by = (2 * j + yo + N - reach) >> 3
        return mask[bx][by:by + 1, :]

    def write_hidden(i, j, xo, yo, v):
        m = mask_of(i, j, xo, yo, H - 1)
        hid_put(2 * i + xo, 2 * j + yo, (jnp.maximum(v + b1[...], 0.0) * m).astype(BF))

    def write_two(i, j, xo, yo, v):
        m = mask_of(i, j, xo, yo, H - 2)
        grad, pick = ups_at(i, j)
        live = (pick == odd + float(4 * xo + 2 * yo)) & (v + b2[...] > 0.0)
        two_put(2 * i + xo, 2 * j + yo, jnp.where(live, grad * m, 0.0).astype(BF))

    def write_one(i, j, xo, yo, v):
        h = hid_at(2 * i + xo + 2, 2 * j + yo + 2).astype(F32)
        one_put(2 * i + xo, 2 * j + yo, jnp.where(h > 0.0, v, 0.0).astype(BF))

    return write_hidden, write_two, write_one


def putter(ref, index):
    def put(x, y, v):
        ref[index(x), cell(y), :] = v

    return put


def upstream(ups, index):
    def ups_at(i, j):
        return ups[index(i), cell(j), 0:Z], ups[index(i), cell(j), Z:2 * Z]

    return ups_at


def term(x, bias, src_at, off_s, delta_at, off_d, acc):
    rights = []
    for y in range(N):
        d = delta_at(x + off_d, y + off_d).astype(F32)
        bias[...] += d
        rights.append(jnp.concatenate([before(d), d, after(d)], axis=0).astype(BF))
    left = jnp.concatenate(
        [jnp.concatenate([src_at(x + off_s + a, y + off_s, 3) for y in range(N)], axis=1)
         for a in range(3)], axis=0)
    acc[...] += lax.dot_general(left, jnp.concatenate(rights, axis=1), (((1,), (1,)), ((), ())),
                                preferred_element_type=F32)


def middle(feat, pool, mask, t1, t2, f2, b1, b2, hid, two, one, acc1, acc2, s1, s2, ups):
    spread = spreader()
    for p in range(2):
        ups[p] = jnp.dot(pool[1 + p], spread, preferred_element_type=F32)
    feat_at, hid_at, two_at, one_at = planes(feat, 4), planes(hid, 4), planes(two, 4), planes(one, 4)
    mid = lambda x: x - 4
    write_hidden, write_two, write_one = writers(
        mask, b1, b2, upstream(ups, lambda i: i - 2), hid_at,
        putter(hid, mid), putter(two, mid), putter(one, mid))
    for ref in (acc1, acc2, s1, s2):
        ref[...] = jnp.zeros_like(ref)
    for i in (2, 3, 4):
        conv_pair(feat_at, 2 * i, t1, W - 2, write_hidden, i)
    for i in (2, 3):
        conv_pair(hid_at, 2 * i, t2, W - 4, write_two, i)
    conv_pair(two_at, 4, f2, W - 6, write_one, 2)
    for x in range(2, 6):
        term(x, s2, hid_at, H - 2, two_at, H - 2, acc2)
    for x in range(3, 5):
        term(x, s1, feat_at, H - 1, one_at, H - 3, acc1)


def outer(mfeat, mpool, xlow, xhigh, clow, chigh, mhid, mtwo, mone, macc1, macc2, ms1, ms2, mask,
          t1, t2, f2, b1, b2, one, parts, hid, two, ups, acc1, acc2, s1, s2):
    def feat_at(x, y, n=1):
        if H <= x < H + N:
            return mfeat[x - H, cell(y, n), :]
        side, corner, k = (xlow, clow, x) if x < H else (xhigh, chigh, x - H - N)
        cells = []
        for v in range(y, y + n):
            if H <= v < H + N:
                cells.append(side[k * N + v - H])
            else:
                cells.append(corner[k * N + (v if v < H else v - N)])
        return jnp.concatenate(cells, axis=0)

    spread = spreader()
    for row, side, corner in ((0, xlow, clow), (3, xhigh, chigh)):
        for y in range(Q + 2):
            if 1 <= y <= Q:
                given = side[N * H + y - 1]
            else:
                given = corner[N * H + (y > 0)]
            ups[row, cell(y), :] = jnp.dot(given, spread, preferred_element_type=F32)
    ups[1] = jnp.dot(mpool[0], spread, preferred_element_type=F32)
    ups[2] = jnp.dot(mpool[Q - 1], spread, preferred_element_type=F32)

    def merged(ref, mid, count):
        def rows_at(x, y, n=1):
            if 4 <= x < 4 + count:
                return mid[x - 4, cell(y, n), :]
            return ref[x if x < 4 else x - count, cell(y, n), :]

        return rows_at

    hid_at, two_at = merged(hid, mhid, 6), merged(two, mtwo, 4)
    one_at = planes(one)
    for x in range(2):
        one[4 + x] = mone[x]
    write_hidden, write_two, write_one = writers(
        mask, b1, b2, upstream(ups, lambda i: i if i < 2 else i - 2), hid_at,
        putter(hid, lambda x: x if x < 4 else x - 6),
        putter(two, lambda x: x if x < 4 else x - 4), putter(one, lambda x: x))
    acc1[...] = macc1[...]
    acc2[...] = macc2[...]
    s1[...] = ms1[...]
    s2[...] = ms2[...]
    for i in (0, 1, 5, 6):
        conv_pair(feat_at, 2 * i, t1, W - 2, write_hidden, i)
    for i in (0, 1, 4, 5):
        conv_pair(hid_at, 2 * i, t2, W - 4, write_two, i)
    for i in (0, 1, 3, 4):
        conv_pair(two_at, 2 * i, f2, W - 6, write_one, i)
    for x in (0, 1, 6, 7):
        term(x, s2, hid_at, H - 2, two_at, H - 2, acc2)
    for x in (0, 1, 2, 5, 6, 7):
        term(x, s1, feat_at, H - 1, one_at, H - 3, acc1)
    rows9 = 9 * C
    pad = jnp.zeros((rows9, Z - 3 * C), F32)
    for k, (acc, sums) in enumerate(((acc1, s1), (acc2, s2))):
        parts[k * rows9:(k + 1) * rows9, :] = jnp.concatenate([acc[...], pad], axis=1).astype(BF)
        total = jnp.sum(sums[...], axis=1, keepdims=True)
        parts[2 * rows9 + k * C:2 * rows9 + (k + 1) * C, :] = jnp.broadcast_to(
            total, (C, Z)).astype(BF)
    rest = parts.shape[0] - 20 * C
    parts[20 * C:, :] = jnp.zeros((rest, Z), BF)


def add_up(got, out):
    total = jnp.sum(got[...].astype(F32), axis=0, keepdims=True).astype(BF)
    out[...] = jnp.broadcast_to(total, out.shape)


def unpack(summed, w1, w2, b1, b2):
    scale = 1.0 / math.sqrt(CELLS)
    rows9 = 9 * C
    for k, (w, b) in enumerate(((w1, b1), (w2, b2))):
        for n in range(9):
            rows = slice(k * rows9 + n * C, k * rows9 + (n + 1) * C)
            block = jnp.transpose(summed[rows, :].astype(F32) * scale)
            for c in range(3):
                w[n * 3 + c] = block[c * C:(c + 1) * C, :]
        rows = slice(2 * rows9 + k * C, 2 * rows9 + (k + 1) * C)
        b[...] = jnp.transpose(summed[rows, :].astype(F32) * scale)[0:1, :]


def final(one, mask, f1, out):
    def write_out(i, j, xo, yo, v):
        out[2 * i + xo, cell(2 * j + yo), :] = (v * mask[1][1:2, :]).astype(BF)

    for i in range(N // 2):
        conv_pair(planes(one), 2 * i, f1, N, write_out, i)


def steps(features, occupancy, weight_one, bias_one, weight_two, bias_two, grad_pooled, pool_choice):
    axes = ("gx", "gy")
    devices = lax.axis_size("gx") * lax.axis_size("gy")
    flags = jnp.pad(occupancy, ((1, 1), (1, 1), (0, 0)))
    window = lax.dynamic_slice(
        flags, (lax.axis_index("gx"), lax.axis_index("gy"), jnp.int32(0)), (3, 3, occupancy.shape[2]))
    mask = jnp.repeat(window, 8, axis=2).astype(F32)
    own = (features * mask[1, 1].astype(BF)).transpose(1, 2, 0, 3).reshape(N, N * C, Z)
    mask = jnp.pad(mask, ((0, 0), (0, 5), (0, 0)))
    pown = jnp.concatenate([grad_pooled, pool_choice.astype(BF)], axis=3)
    pown = pown.transpose(1, 2, 0, 3).reshape(Q, Q * C, Z)

    face = ((N * H + Q, C, Z), BF)
    ydown, yup, xdown, xup = call(pack_faces, [face] * 4)(own, pown)
    ylow = shift(ydown, "gy", 1)
    yhigh = shift(yup, "gy", -1)
    xlow = shift(xdown, "gx", 1)
    xhigh = shift(xup, "gx", -1)

    def blocks(weight):
        return weight.transpose(1, 2, 3, 0, 4).reshape(27, C, C)

    t1, t2, f2, f1, b1, b2 = call(
        prepare, [((6 * C, 12 * C), BF)] * 4 + [((C, Z), F32)] * 2)(
            blocks(weight_one), blocks(weight_two),
            bias_one.reshape(1, C), bias_two.reshape(1, C))

    own, pown, t1 = lax.optimization_barrier((own, pown, t1))
    mfeat, mpool, cdown, cup = call(
        pack_corners,
        [((N, W * C, Z), BF), ((Q, (Q + 2) * C, Z), BF)] + [((N * H + 2, C, Z), BF)] * 2)(own, pown, ylow, yhigh)
    clow = shift(cdown, "gx", 1)
    chigh = shift(cup, "gx", -1)

    grads = [((9 * C, 3 * C), F32)] * 2 + [((C, Z), F32)] * 2
    mids = call(
        middle,
        [((6, (W - 2) * C, Z), BF), ((4, (W - 4) * C, Z), BF), ((2, (W - 6) * C, Z), BF)] + grads,
        [((2, (Q + 2) * C, 2 * Z), F32)])(mfeat, mpool, mask, t1, t2, f2, b1, b2)

    one, parts = call(
        outer, [((W - 6, (W - 6) * C, Z), BF), ((devices * ROWS, Z), BF)],
        [((8, (W - 2) * C, Z), BF), ((8, (W - 4) * C, Z), BF),
         ((4, (Q + 2) * C, 2 * Z), F32)] + grads)(mfeat, mpool, xlow, xhigh, clow, chigh, *mids, mask, t1, t2, f2, b1, b2)

    block = (devices, ROWS, Z)
    got = lax.all_to_all(parts.reshape(block), axes, 0, 0, tiled=True)
    out, = call(final, [((N, N * C, Z), BF)])(one, mask, f1)
    mine, = call(add_up, [(block, BF)])(got)
    summed = lax.all_to_all(mine, axes, 0, 0, tiled=True).reshape(devices * ROWS, Z)
    gw1, gw2, gb1, gb2 = call(
        unpack, [((27, C, C), F32)] * 2 + [((1, C), F32)] * 2)(summed)

    def weights(g):
        return g.reshape(3, 3, 3, C, C).transpose(3, 0, 1, 2, 4)

    grad_input = out.reshape(N, N, C, Z).transpose(2, 0, 1, 3)
    return grad_input, weights(gw1), gb1.reshape(C), weights(gw2), gb2.reshape(C)


def solution(mesh):
    cells = P(None, "gx", "gy", None)
    return jax.shard_map(
        steps,
        mesh=mesh,
        in_specs=(cells, P(), P(), P(), P(), P(), cells, cells),
        out_specs=(cells, P(), P(), P(), P()),
        check_vma=False,
    )
```

```python
import math

import jax
import jax.numpy as jnp
from jax import lax
from jax.experimental import pallas as pl
from jax.experimental.pallas import tpu as pltpu
from jax.sharding import PartitionSpec as P


BF = jnp.bfloat16
F32 = jnp.float32
C, Z, N, H = 32, 128, 8, 4
W = N + 2 * H
Q = N // 2
ROWS = 8
CELLS = 128 * 64 * 128


def call(kernel, outs, scratch=()):
    return pl.pallas_call(
        kernel,
        out_shape=tuple(jax.ShapeDtypeStruct(s, d) for s, d in outs),
        scratch_shapes=[pltpu.VMEM(s, d) for s, d in scratch],
        compiler_params=pltpu.CompilerParams(vmem_limit_bytes=40 << 20),
    )


def shift(v, axis, step):
    devices = lax.axis_size(axis)
    pairs = [(i, i + step) for i in range(devices) if 0 <= i + step < devices]
    return lax.ppermute(v, axis, pairs)


def swap(v, axis, first):
    pairs = []
    for i in range(first, lax.axis_size(axis) - 1, 2):
        pairs += [(i, i + 1), (i + 1, i)]
    return lax.ppermute(v, axis, pairs)


def odd_place():
    return lax.axis_index("gx") % 2


def cell(y, n=1):
    return slice(y * C, (y + n) * C)


def prepare(w1, w2, b1, b2, t1, t2, f2, f1, c1, c2):
    zero = jnp.zeros((C, C), F32)
    for src, plain, flip in ((w1, t1, f1), (w2, t2, f2)):
        for a in range(3):
            for c in range(3):
                rows = slice(c * C, (c + 1) * C)
                high = slice((3 + c) * C, (4 + c) * C)
                cols = slice(a * 4 * C, (a + 1) * 4 * C)
                line = jnp.concatenate(
                    [src[a * 9 + b * 3 + c].astype(F32) for b in range(3)] + [zero], axis=1)
                plain[rows, cols] = line.astype(BF)
                plain[high, cols] = pltpu.roll(line, C, 1).astype(BF)
                tall = jnp.concatenate(
                    [src[(2 - a) * 9 + (2 - b) * 3 + 2 - c].astype(F32) for b in range(3)] + [zero],
                    axis=0)
                line = jnp.transpose(tall)
                flip[rows, cols] = line.astype(BF)
                flip[high, cols] = pltpu.roll(line, C, 1).astype(BF)
    for src, dst in ((b1, c1), (b2, c2)):
        dst[...] = jnp.transpose(jnp.broadcast_to(src[...], (Z, C)))


def pack_faces(own, pown, ylow, yhigh, near, far):
    odd = odd_place()
    for x in range(N):
        for k in range(H):
            ylow[x * H + k] = own[x, cell(N - H + k), :]
            yhigh[x * H + k] = own[x, cell(k), :]
    for q in range(Q):
        ylow[N * H + q] = pown[q, cell(Q - 1), :]
        yhigh[N * H + q] = pown[q, cell(0), :]
    for ref, low in ((near, odd), (far, 1 - odd)):
        for k in range(H):
            for y in range(N):
                ref[k * N + y] = own[(N - H) * (1 - low) + k, cell(y), :]
        for q in range(Q):
            ref[N * H + q] = pown[(Q - 1) * (1 - low), cell(q), :]


def pack_corners(own, pown, ylow, yhigh, feat, pool, near, far):
    odd = odd_place()
    for ref, low in ((near, odd), (far, 1 - odd)):
        for x in range(H):
            for k in range(H):
                at = ((N - H) * (1 - low) + x) * H + k
                ref[x * N + k] = ylow[at]
                ref[x * N + H + k] = yhigh[at]
        at = N * H + (Q - 1) * (1 - low)
        ref[N * H] = ylow[at]
        ref[N * H + 1] = yhigh[at]
    for x in range(N):
        feat[x, cell(H, N), :] = own[x]
        for k in range(H):
            feat[x, cell(k), :] = ylow[x * H + k]
            feat[x, cell(H + N + k), :] = yhigh[x * H + k]
    for x in range(Q):
        pool[x, cell(1, Q), :] = pown[x]
        pool[x, cell(0), :] = ylow[N * H + x]
        pool[x, cell(Q + 1), :] = yhigh[N * H + x]


def after(v):
    lane = lax.broadcasted_iota(jnp.int32, v.shape, 1)
    return jnp.where(lane == 0, 0.0, pltpu.roll(v, 1, 1))


def before(v):
    lane = lax.broadcasted_iota(jnp.int32, v.shape, 1)
    return jnp.where(lane == Z - 1, 0.0, pltpu.roll(v, Z - 1, 1))


def spreader():
    row = lax.broadcasted_iota(jnp.int32, (Z, 2 * Z), 0)
    col = lax.broadcasted_iota(jnp.int32, (Z, 2 * Z), 1)
    return jnp.where(row == col // 2, 1.0, 0.0).astype(BF)


def conv_pair(rows_at, x, weight, width, write, i):
    for j in range(width // 2):
        rows = [rows_at(x + d, 2 * j, 4) for d in range(4)]
        tile = jnp.concatenate(
            [jnp.concatenate([rows[d], rows[d + 1]], axis=1) for d in range(3)], axis=0)
        got = jnp.dot(weight[...], tile, preferred_element_type=F32)
        for xo in range(2):
            for yo in range(2):
                g = got[yo * 3 * C:(yo + 1) * 3 * C, xo * Z:(xo + 1) * Z]
                v = g[C:2 * C] + after(g[0:C]) + before(g[2 * C:])
                write(i, j, xo, yo, v)


def planes(ref, first=0):
    def rows_at(x, y, n=1):
        return ref[x - first, cell(y, n), :]

    return rows_at


def writers(mask, b1, b2, ups_at, hid_at, hid_put, two_put, one_put):
    lane = lax.broadcasted_iota(jnp.int32, (C, Z), 1)
    odd = (lane % 2).astype(F32)

    def mask_of(i, j, xo, yo, reach):
        bx = (2 * i + xo + N - reach) >> 3
        by = (2 * j + yo + N - reach) >> 3
        return mask[bx][by:by + 1, :]

    def write_hidden(i, j, xo, yo, v):
        m = mask_of(i, j, xo, yo, H - 1)
        hid_put(2 * i + xo, 2 * j + yo, (jnp.maximum(v + b1[...], 0.0) * m).astype(BF))

    def write_two(i, j, xo, yo, v):
        m = mask_of(i, j, xo, yo, H - 2)
        grad, pick = ups_at(i, j)
        live = (pick == odd + float(4 * xo + 2 * yo)) & (v + b2[...] > 0.0)
        two_put(2 * i + xo, 2 * j + yo, jnp.where(live, grad * m, 0.0).astype(BF))

    def write_one(i, j, xo, yo, v):
        h = hid_at(2 * i + xo + 2, 2 * j + yo + 2).astype(F32)
        one_put(2 * i + xo, 2 * j + yo, jnp.where(h > 0.0, v, 0.0).astype(BF))

    return write_hidden, write_two, write_one


def putter(ref, index):
    def put(x, y, v):
        ref[index(x), cell(y), :] = v

    return put


def upstream(ups, index):
    def ups_at(i, j):
        return ups[index(i), cell(j), 0:Z], ups[index(i), cell(j), Z:2 * Z]

    return ups_at


def term(x, bias, src_at, off_s, delta_at, off_d, acc):
    rights = []
    for y in range(N):
        d = delta_at(x + off_d, y + off_d).astype(F32)
        bias[...] += d
        rights.append(jnp.concatenate([before(d), d, after(d)], axis=0).astype(BF))
    left = jnp.concatenate(
        [jnp.concatenate([src_at(x + off_s + a, y + off_s, 3) for y in range(N)], axis=1)
         for a in range(3)], axis=0)
    acc[...] += lax.dot_general(left, jnp.concatenate(rights, axis=1), (((1,), (1,)), ((), ())),
                                preferred_element_type=F32)


def middle(feat, pool, mask, t1, t2, f2, b1, b2, hid, two, one, acc1, acc2, s1, s2, ups):
    spread = spreader()
    for p in range(2):
        ups[p] = jnp.dot(pool[1 + p], spread, preferred_element_type=F32)
    feat_at, hid_at, two_at, one_at = planes(feat, 4), planes(hid, 4), planes(two, 4), planes(one, 4)
    mid = lambda x: x - 4
    write_hidden, write_two, write_one = writers(
        mask, b1, b2, upstream(ups, lambda i: i - 2), hid_at,
        putter(hid, mid), putter(two, mid), putter(one, mid))
    for ref in (acc1, acc2, s1, s2):
        ref[...] = jnp.zeros_like(ref)
    for i in (2, 3, 4):
        conv_pair(feat_at, 2 * i, t1, W - 2, write_hidden, i)
    for i in (2, 3):
        conv_pair(hid_at, 2 * i, t2, W - 4, write_two, i)
    conv_pair(two_at, 4, f2, W - 6, write_one, 2)
    for x in range(2, 6):
        term(x, s2, hid_at, H - 2, two_at, H - 2, acc2)
    for x in range(3, 5):
        term(x, s1, feat_at, H - 1, one_at, H - 3, acc1)


def outer(mfeat, mpool, xnear, xfar, cnear, cfar, mhid, mtwo, mone, macc1, macc2, ms1, ms2, mask,
          t1, t2, f2, b1, b2, one, parts, xlow, xhigh, clow, chigh, hid, two, ups, acc1, acc2, s1, s2):
    odd = odd_place()

    @pl.when(odd == 0)
    def _():
        xlow[...], xhigh[...] = xfar[...], xnear[...]
        clow[...], chigh[...] = cfar[...], cnear[...]

    @pl.when(odd == 1)
    def _():
        xlow[...], xhigh[...] = xnear[...], xfar[...]
        clow[...], chigh[...] = cnear[...], cfar[...]

    def feat_at(x, y, n=1):
        if H <= x < H + N:
            return mfeat[x - H, cell(y, n), :]
        side, corner, k = (xlow, clow, x) if x < H else (xhigh, chigh, x - H - N)
        cells = []
        for v in range(y, y + n):
            if H <= v < H + N:
                cells.append(side[k * N + v - H])
            else:
                cells.append(corner[k * N + (v if v < H else v - N)])
        return jnp.concatenate(cells, axis=0)

    spread = spreader()
    for row, side, corner in ((0, xlow, clow), (3, xhigh, chigh)):
        for y in range(Q + 2):
            if 1 <= y <= Q:
                given = side[N * H + y - 1]
            else:
                given = corner[N * H + (y > 0)]
            ups[row, cell(y), :] = jnp.dot(given, spread, preferred_element_type=F32)
    ups[1] = jnp.dot(mpool[0], spread, preferred_element_type=F32)
    ups[2] = jnp.dot(mpool[Q - 1], spread, preferred_element_type=F32)

    def merged(ref, mid, count):
        def rows_at(x, y, n=1):
            if 4 <= x < 4 + count:
                return mid[x - 4, cell(y, n), :]
            return ref[x if x < 4 else x - count, cell(y, n), :]

        return rows_at

    hid_at, two_at = merged(hid, mhid, 6), merged(two, mtwo, 4)
    one_at = planes(one)
    for x in range(2):
        one[4 + x] = mone[x]
    write_hidden, write_two, write_one = writers(
        mask, b1, b2, upstream(ups, lambda i: i if i < 2 else i - 2), hid_at,
        putter(hid, lambda x: x if x < 4 else x - 6),
        putter(two, lambda x: x if x < 4 else x - 4), putter(one, lambda x: x))
    acc1[...] = macc1[...]
    acc2[...] = macc2[...]
    s1[...] = ms1[...]
    s2[...] = ms2[...]
    for i in (0, 1, 5, 6):
        conv_pair(feat_at, 2 * i, t1, W - 2, write_hidden, i)
    for i in (0, 1, 4, 5):
        conv_pair(hid_at, 2 * i, t2, W - 4, write_two, i)
    for i in (0, 1, 3, 4):
        conv_pair(two_at, 2 * i, f2, W - 6, write_one, i)
    for x in (0, 1, 6, 7):
        term(x, s2, hid_at, H - 2, two_at, H - 2, acc2)
    for x in (0, 1, 2, 5, 6, 7):
        term(x, s1, feat_at, H - 1, one_at, H - 3, acc1)
    rows9 = 9 * C
    pad = jnp.zeros((rows9, Z - 3 * C), F32)
    for k, (acc, sums) in enumerate(((acc1, s1), (acc2, s2))):
        parts[k * rows9:(k + 1) * rows9, :] = jnp.concatenate([acc[...], pad], axis=1).astype(BF)
        total = jnp.sum(sums[...], axis=1, keepdims=True)
        parts[2 * rows9 + k * C:2 * rows9 + (k + 1) * C, :] = jnp.broadcast_to(
            total, (C, Z)).astype(BF)
    rest = parts.shape[0] - 20 * C
    parts[20 * C:, :] = jnp.zeros((rest, Z), BF)


def add_up(got, out):
    total = jnp.sum(got[...].astype(F32), axis=0, keepdims=True).astype(BF)
    out[...] = jnp.broadcast_to(total, out.shape)


def unpack(summed, w1, w2, b1, b2):
    scale = 1.0 / math.sqrt(CELLS)
    rows9 = 9 * C
    for k, (w, b) in enumerate(((w1, b1), (w2, b2))):
        for n in range(9):
            rows = slice(k * rows9 + n * C, k * rows9 + (n + 1) * C)
            block = jnp.transpose(summed[rows, :].astype(F32) * scale)
            for c in range(3):
                w[n * 3 + c] = block[c * C:(c + 1) * C, :]
        rows = slice(2 * rows9 + k * C, 2 * rows9 + (k + 1) * C)
        b[...] = jnp.transpose(summed[rows, :].astype(F32) * scale)[0:1, :]


def final(one, mask, f1, out):
    def write_out(i, j, xo, yo, v):
        out[2 * i + xo, cell(2 * j + yo), :] = (v * mask[1][1:2, :]).astype(BF)

    for i in range(N // 2):
        conv_pair(planes(one), 2 * i, f1, N, write_out, i)


def steps(features, occupancy, weight_one, bias_one, weight_two, bias_two, grad_pooled, pool_choice):
    axes = ("gx", "gy")
    devices = lax.axis_size("gx") * lax.axis_size("gy")
    flags = jnp.pad(occupancy, ((1, 1), (1, 1), (0, 0)))
    window = lax.dynamic_slice(
        flags, (lax.axis_index("gx"), lax.axis_index("gy"), jnp.int32(0)), (3, 3, occupancy.shape[2]))
    mask = jnp.repeat(window, 8, axis=2).astype(F32)
    own = (features * mask[1, 1].astype(BF)).transpose(1, 2, 0, 3).reshape(N, N * C, Z)
    mask = jnp.pad(mask, ((0, 0), (0, 5), (0, 0)))
    pown = jnp.concatenate([grad_pooled, pool_choice.astype(BF)], axis=3)
    pown = pown.transpose(1, 2, 0, 3).reshape(Q, Q * C, Z)

    face = ((N * H + Q, C, Z), BF)
    ydown, yup, near, far = call(pack_faces, [face] * 4)(own, pown)
    ylow = shift(ydown, "gy", 1)
    yhigh = shift(yup, "gy", -1)
    xfar = swap(far, "gx", 1)
    xnear = swap(near, "gx", 0)

    def blocks(weight):
        return weight.transpose(1, 2, 3, 0, 4).reshape(27, C, C)

    t1, t2, f2, f1, b1, b2 = call(
        prepare, [((6 * C, 12 * C), BF)] * 4 + [((C, Z), F32)] * 2)(
            blocks(weight_one), blocks(weight_two),
            bias_one.reshape(1, C), bias_two.reshape(1, C))

    own, pown, t1 = lax.optimization_barrier((own, pown, t1))
    corner = ((N * H + 2, C, Z), BF)
    mfeat, mpool, near, far = call(
        pack_corners,
        [((N, W * C, Z), BF), ((Q, (Q + 2) * C, Z), BF)] + [corner] * 2)(own, pown, ylow, yhigh)
    cfar = swap(far, "gx", 1)
    cnear = swap(near, "gx", 0)

    grads = [((9 * C, 3 * C), F32)] * 2 + [((C, Z), F32)] * 2
    mids = call(
        middle,
        [((6, (W - 2) * C, Z), BF), ((4, (W - 4) * C, Z), BF), ((2, (W - 6) * C, Z), BF)] + grads,
        [((2, (Q + 2) * C, 2 * Z), F32)])(mfeat, mpool, mask, t1, t2, f2, b1, b2)

    one, parts = call(
        outer, [((W - 6, (W - 6) * C, Z), BF), ((devices * ROWS, Z), BF)],
        [face, face, corner, corner, ((8, (W - 2) * C, Z), BF), ((8, (W - 4) * C, Z), BF),
         ((4, (Q + 2) * C, 2 * Z), F32)] + grads)(mfeat, mpool, xnear, xfar, cnear, cfar, *mids, mask, t1, t2, f2, b1, b2)

    block = (devices, ROWS, Z)
    got = lax.all_to_all(parts.reshape(block), axes, 0, 0, tiled=True)
    out, = call(final, [((N, N * C, Z), BF)])(one, mask, f1)
    mine, = call(add_up, [(block, BF)])(got)
    summed = lax.all_to_all(mine, axes, 0, 0, tiled=True).reshape(devices * ROWS, Z)
    gw1, gw2, gb1, gb2 = call(
        unpack, [((27, C, C), F32)] * 2 + [((1, C), F32)] * 2)(summed)

    def weights(g):
        return g.reshape(3, 3, 3, C, C).transpose(3, 0, 1, 2, 4)

    grad_input = out.reshape(N, N, C, Z).transpose(2, 0, 1, 3)
    return grad_input, weights(gw1), gb1.reshape(C), weights(gw2), gb2.reshape(C)


def solution(mesh):
    cells = P(None, "gx", "gy", None)
    return jax.shard_map(
        steps,
        mesh=mesh,
        in_specs=(cells, P(), P(), P(), P(), P(), cells, cells),
        out_specs=(cells, P(), P(), P(), P()),
        check_vma=False,
    )
```

```python
import math

import jax
import jax.numpy as jnp
from jax import lax
from jax.experimental import pallas as pl
from jax.experimental.pallas import tpu as pltpu
from jax.sharding import PartitionSpec as P


BF = jnp.bfloat16
F32 = jnp.float32
C, Z, N, H = 32, 128, 8, 4
W = N + 2 * H
Q = N // 2
ROWS = 8
CELLS = 128 * 64 * 128


def call(kernel, outs, scratch=()):
    return pl.pallas_call(
        kernel,
        out_shape=tuple(jax.ShapeDtypeStruct(s, d) for s, d in outs),
        scratch_shapes=[pltpu.VMEM(s, d) for s, d in scratch],
        compiler_params=pltpu.CompilerParams(vmem_limit_bytes=40 << 20),
    )


def shift(v, axis, step):
    devices = lax.axis_size(axis)
    pairs = [(i, i + step) for i in range(devices) if 0 <= i + step < devices]
    return lax.ppermute(v, axis, pairs)


def swap(v, axis, first):
    pairs = []
    for i in range(first, lax.axis_size(axis) - 1, 2):
        pairs += [(i, i + 1), (i + 1, i)]
    return lax.ppermute(v, axis, pairs)


def odd_place():
    return lax.axis_index("gx") % 2


def cell(y, n=1):
    return slice(y * C, (y + n) * C)


def prepare(w1, w2, b1, b2, t1, t2, f2, f1, c1, c2):
    zero = jnp.zeros((C, C), F32)
    for src, plain, flip in ((w1, t1, f1), (w2, t2, f2)):
        for a in range(3):
            for c in range(3):
                rows = slice(c * C, (c + 1) * C)
                high = slice((3 + c) * C, (4 + c) * C)
                cols = slice(a * 4 * C, (a + 1) * 4 * C)
                line = jnp.concatenate(
                    [src[a * 9 + b * 3 + c].astype(F32) for b in range(3)] + [zero], axis=1)
                plain[rows, cols] = line.astype(BF)
                plain[high, cols] = pltpu.roll(line, C, 1).astype(BF)
                tall = jnp.concatenate(
                    [src[(2 - a) * 9 + (2 - b) * 3 + 2 - c].astype(F32) for b in range(3)] + [zero],
                    axis=0)
                line = jnp.transpose(tall)
                flip[rows, cols] = line.astype(BF)
                flip[high, cols] = pltpu.roll(line, C, 1).astype(BF)
    for src, dst in ((b1, c1), (b2, c2)):
        dst[...] = jnp.transpose(jnp.broadcast_to(src[...], (Z, C)))


def pack_faces(own, pown, ylow, yhigh, near, far):
    odd = odd_place()
    for x in range(N):
        for k in range(H):
            ylow[x * H + k] = own[x, cell(N - H + k), :]
            yhigh[x * H + k] = own[x, cell(k), :]
    for q in range(Q):
        ylow[N * H + q] = pown[q, cell(Q - 1), :]
        yhigh[N * H + q] = pown[q, cell(0), :]
    for ref, low in ((near, odd), (far, 1 - odd)):
        for k in range(H):
            for y in range(N):
                ref[k * N + y] = own[(N - H) * (1 - low) + k, cell(y), :]
        for q in range(Q):
            ref[N * H + q] = pown[(Q - 1) * (1 - low), cell(q), :]


def pack_corners(own, pown, ylow, yhigh, feat, pool, near, far):
    odd = odd_place()
    for ref, low in ((near, odd), (far, 1 - odd)):
        for x in range(H):
            for k in range(H):
                at = ((N - H) * (1 - low) + x) * H + k
                ref[x * N + k] = ylow[at]
                ref[x * N + H + k] = yhigh[at]
        at = N * H + (Q - 1) * (1 - low)
        ref[N * H] = ylow[at]
        ref[N * H + 1] = yhigh[at]
    for x in range(N):
        feat[x, cell(H, N), :] = own[x]
        for k in range(H):
            feat[x, cell(k), :] = ylow[x * H + k]
            feat[x, cell(H + N + k), :] = yhigh[x * H + k]
    for x in range(Q):
        pool[x, cell(1, Q), :] = pown[x]
        pool[x, cell(0), :] = ylow[N * H + x]
        pool[x, cell(Q + 1), :] = yhigh[N * H + x]


def after(v):
    lane = lax.broadcasted_iota(jnp.int32, v.shape, 1)
    return jnp.where(lane == 0, 0.0, pltpu.roll(v, 1, 1))


def before(v):
    lane = lax.broadcasted_iota(jnp.int32, v.shape, 1)
    return jnp.where(lane == Z - 1, 0.0, pltpu.roll(v, Z - 1, 1))


def spreader():
    row = lax.broadcasted_iota(jnp.int32, (Z, 2 * Z), 0)
    col = lax.broadcasted_iota(jnp.int32, (Z, 2 * Z), 1)
    return jnp.where(row == col // 2, 1.0, 0.0).astype(BF)


def conv_pair(rows_at, x, weight, pairs, write, i):
    for j in pairs:
        rows = [rows_at(x + d, 2 * j, 4) for d in range(4)]
        tile = jnp.concatenate(
            [jnp.concatenate([rows[d], rows[d + 1]], axis=1) for d in range(3)], axis=0)
        got = jnp.dot(weight[...], tile, preferred_element_type=F32)
        for xo in range(2):
            for yo in range(2):
                g = got[yo * 3 * C:(yo + 1) * 3 * C, xo * Z:(xo + 1) * Z]
                v = g[C:2 * C] + after(g[0:C]) + before(g[2 * C:])
                write(i, j, xo, yo, v)


def planes(ref, first=0):
    def rows_at(x, y, n=1):
        return ref[x - first, cell(y, n), :]

    return rows_at


def writers(mask, b1, b2, ups_at, hid_at, hid_put, two_put, one_put):
    lane = lax.broadcasted_iota(jnp.int32, (C, Z), 1)
    odd = (lane % 2).astype(F32)

    def mask_of(i, j, xo, yo, reach):
        bx = (2 * i + xo + N - reach) >> 3
        by = (2 * j + yo + N - reach) >> 3
        return mask[bx][by:by + 1, :]

    def write_hidden(i, j, xo, yo, v):
        m = mask_of(i, j, xo, yo, H - 1)
        hid_put(2 * i + xo, 2 * j + yo, (jnp.maximum(v + b1[...], 0.0) * m).astype(BF))

    def write_two(i, j, xo, yo, v):
        m = mask_of(i, j, xo, yo, H - 2)
        grad, pick = ups_at(i, j)
        live = (pick == odd + float(4 * xo + 2 * yo)) & (v + b2[...] > 0.0)
        two_put(2 * i + xo, 2 * j + yo, jnp.where(live, grad * m, 0.0).astype(BF))

    def write_one(i, j, xo, yo, v):
        h = hid_at(2 * i + xo + 2, 2 * j + yo + 2).astype(F32)
        one_put(2 * i + xo, 2 * j + yo, jnp.where(h > 0.0, v, 0.0).astype(BF))

    return write_hidden, write_two, write_one


def putter(ref, index):
    def put(x, y, v):
        ref[index(x), cell(y), :] = v

    return put


def upstream(ups, index):
    def ups_at(i, j):
        return ups[index(i), cell(j), 0:Z], ups[index(i), cell(j), Z:2 * Z]

    return ups_at


def term(x, ys, bias, src_at, off_s, delta_at, off_d, acc):
    rights = []
    for y in ys:
        d = delta_at(x + off_d, y + off_d).astype(F32)
        bias[...] += d
        rights.append(jnp.concatenate([before(d), d, after(d)], axis=0).astype(BF))
    left = jnp.concatenate(
        [jnp.concatenate([src_at(x + off_s + a, y + off_s, 3) for y in ys], axis=1)
         for a in range(3)], axis=0)
    acc[...] += lax.dot_general(left, jnp.concatenate(rights, axis=1), (((1,), (1,)), ((), ())),
                                preferred_element_type=F32)


def middle(feat, pool, mask, t1, t2, f2, b1, b2, hid, two, one, acc1, acc2, s1, s2, ups):
    spread = spreader()
    for p in range(2):
        ups[p] = jnp.dot(pool[1 + p], spread, preferred_element_type=F32)
    feat_at, hid_at, two_at, one_at = planes(feat, 4), planes(hid, 4), planes(two, 4), planes(one, 4)
    mid = lambda x: x - 4
    write_hidden, write_two, write_one = writers(
        mask, b1, b2, upstream(ups, lambda i: i - 2), hid_at,
        putter(hid, mid), putter(two, mid), putter(one, mid))
    for ref in (acc1, acc2, s1, s2):
        ref[...] = jnp.zeros_like(ref)
    for i in (2, 3, 4):
        conv_pair(feat_at, 2 * i, t1, range(W // 2 - 1), write_hidden, i)
    for i in (2, 3):
        conv_pair(hid_at, 2 * i, t2, range(W // 2 - 2), write_two, i)
    conv_pair(two_at, 4, f2, range(W // 2 - 3), write_one, 2)
    for x in range(2, 6):
        term(x, range(N), s2, hid_at, H - 2, two_at, H - 2, acc2)
    for x in range(3, 5):
        term(x, range(N), s1, feat_at, H - 1, one_at, H - 3, acc1)


def packed(x, mid):
    return x if x < 4 else x - mid


def merged(ref, full, mid, inner=None, count=0):
    def one_cell(p, y):
        if 4 <= y < 4 + count:
            return inner[p, cell(y - 4), :]
        return ref[p, cell(y), :]

    def rows_at(x, y, n=1):
        if 4 <= x < 4 + mid:
            return full[x - 4, cell(y, n), :]
        return jnp.concatenate([one_cell(packed(x, mid), v) for v in range(y, y + n)], axis=0)

    return rows_at


def features_at(mfeat, xlow, xhigh, clow, chigh):
    def feat_at(x, y, n=1):
        if H <= x < H + N:
            return mfeat[x - H, cell(y, n), :]
        side, corner, k = (xlow, clow, x) if x < H else (xhigh, chigh, x - H - N)
        cells = []
        for v in range(y, y + n):
            if H <= v < H + N:
                cells.append(side[k * N + v - H])
            else:
                cells.append(corner[k * N + (v if v < H else v - N)])
        return jnp.concatenate(cells, axis=0)

    return feat_at


def resolve(near, far, low, high):
    odd = odd_place()

    @pl.when(odd == 0)
    def _():
        low[...], high[...] = far[...], near[...]

    @pl.when(odd == 1)
    def _():
        low[...], high[...] = near[...], far[...]


def rim(mfeat, mpool, xnear, xfar, mhid, mtwo, mone, macc1, macc2, ms1, ms2, mask,
        t1, t2, f2, b1, b2, xlow, xhigh, hid, two, one, acc1, acc2, s1, s2, ups):
    resolve(xnear, xfar, xlow, xhigh)
    spread = spreader()
    for row, side in ((0, xlow), (3, xhigh)):
        for y in range(2, Q):
            ups[row, cell(y), :] = jnp.dot(
                side[N * H + y - 1], spread, preferred_element_type=F32)
    ups[1] = jnp.dot(mpool[0], spread, preferred_element_type=F32)
    ups[2] = jnp.dot(mpool[Q - 1], spread, preferred_element_type=F32)

    def inner_put(ref, mid):
        def put(x, y, v):
            ref[packed(x, mid), cell(y - 4), :] = v

        return put

    feat_at = features_at(mfeat, xlow, xhigh, None, None)
    hid_at = merged(None, mhid, 6, hid, 6)
    two_at = merged(None, mtwo, 4, two, 4)
    one_at = merged(None, mone, 2, one, 2)
    write_hidden, write_two, write_one = writers(
        mask, b1, b2, upstream(ups, lambda i: packed(i, 2) if i > 3 else i), hid_at,
        inner_put(hid, 6), inner_put(two, 4), inner_put(one, 2))
    for dst, src in ((acc1, macc1), (acc2, macc2), (s1, ms1), (s2, ms2)):
        dst[...] = src[...]
    for i in (0, 1, 5, 6):
        conv_pair(feat_at, 2 * i, t1, (2, 3, 4), write_hidden, i)
    for i in (0, 1, 4, 5):
        conv_pair(hid_at, 2 * i, t2, (2, 3), write_two, i)
    for i in (0, 1, 3, 4):
        conv_pair(two_at, 2 * i, f2, (2,), write_one, i)
    for x in (0, 1, 6, 7):
        term(x, (2, 3, 4, 5), s2, hid_at, H - 2, two_at, H - 2, acc2)
    for x in (0, 1, 2, 5, 6, 7):
        term(x, (3, 4), s1, feat_at, H - 1, one_at, H - 3, acc1)


def outer(mfeat, mpool, cnear, cfar, mhid, mtwo, mone, xlow, xhigh, rhid, rtwo, rone,
          macc1, macc2, ms1, ms2, mask, t1, t2, f2, b1, b2, one, parts,
          clow, chigh, hid, two, ups, acc1, acc2, s1, s2):
    resolve(cnear, cfar, clow, chigh)
    spread = spreader()
    for row, side, corner in ((0, xlow, clow), (3, xhigh, chigh)):
        for y in range(Q + 2):
            if 1 <= y <= Q:
                given = side[N * H + y - 1]
            else:
                given = corner[N * H + (y > 0)]
            ups[row, cell(y), :] = jnp.dot(given, spread, preferred_element_type=F32)
    ups[1] = jnp.dot(mpool[0], spread, preferred_element_type=F32)
    ups[2] = jnp.dot(mpool[Q - 1], spread, preferred_element_type=F32)

    def rim_put(ref, mid):
        return putter(ref, lambda x: packed(x, mid))

    feat_at = features_at(mfeat, xlow, xhigh, clow, chigh)
    hid_at = merged(hid, mhid, 6, rhid, 6)
    two_at = merged(two, mtwo, 4, rtwo, 4)
    one_at = planes(one)
    for x in range(10):
        if 4 <= x < 6:
            one[x] = mone[x - 4]
        else:
            one[x, cell(4, 2), :] = rone[packed(x, 2)]
    write_hidden, write_two, write_one = writers(
        mask, b1, b2, upstream(ups, lambda i: packed(i, 2) if i > 3 else i), hid_at,
        rim_put(hid, 6), rim_put(two, 4), putter(one, lambda x: x))
    acc1[...] = macc1[...]
    acc2[...] = macc2[...]
    s1[...] = ms1[...]
    s2[...] = ms2[...]
    for i in (0, 1, 5, 6):
        conv_pair(feat_at, 2 * i, t1, (0, 1, 5, 6), write_hidden, i)
    for i in (0, 1, 4, 5):
        conv_pair(hid_at, 2 * i, t2, (0, 1, 4, 5), write_two, i)
    for i in (0, 1, 3, 4):
        conv_pair(two_at, 2 * i, f2, (0, 1, 3, 4), write_one, i)
    for x in (0, 1, 6, 7):
        term(x, (0, 1, 6, 7), s2, hid_at, H - 2, two_at, H - 2, acc2)
    for x in (0, 1, 2, 5, 6, 7):
        term(x, (0, 1, 2, 5, 6, 7), s1, feat_at, H - 1, one_at, H - 3, acc1)
    rows9 = 9 * C
    pad = jnp.zeros((rows9, Z - 3 * C), F32)
    for k, (acc, sums) in enumerate(((acc1, s1), (acc2, s2))):
        parts[k * rows9:(k + 1) * rows9, :] = jnp.concatenate([acc[...], pad], axis=1).astype(BF)
        total = jnp.sum(sums[...], axis=1, keepdims=True)
        parts[2 * rows9 + k * C:2 * rows9 + (k + 1) * C, :] = jnp.broadcast_to(
            total, (C, Z)).astype(BF)
    rest = parts.shape[0] - 20 * C
    parts[20 * C:, :] = jnp.zeros((rest, Z), BF)


def add_up(got, out):
    total = jnp.sum(got[...].astype(F32), axis=0, keepdims=True).astype(BF)
    out[...] = jnp.broadcast_to(total, out.shape)


def unpack(summed, w1, w2, b1, b2):
    scale = 1.0 / math.sqrt(CELLS)
    rows9 = 9 * C
    for k, (w, b) in enumerate(((w1, b1), (w2, b2))):
        for n in range(9):
            rows = slice(k * rows9 + n * C, k * rows9 + (n + 1) * C)
            block = jnp.transpose(summed[rows, :].astype(F32) * scale)
            for c in range(3):
                w[n * 3 + c] = block[c * C:(c + 1) * C, :]
        rows = slice(2 * rows9 + k * C, 2 * rows9 + (k + 1) * C)
        b[...] = jnp.transpose(summed[rows, :].astype(F32) * scale)[0:1, :]


def final(one, mask, f1, out):
    def write_out(i, j, xo, yo, v):
        out[2 * i + xo, cell(2 * j + yo), :] = (v * mask[1][1:2, :]).astype(BF)

    for i in range(N // 2):
        conv_pair(planes(one), 2 * i, f1, range(N // 2), write_out, i)


def steps(features, occupancy, weight_one, bias_one, weight_two, bias_two, grad_pooled, pool_choice):
    axes = ("gx", "gy")
    devices = lax.axis_size("gx") * lax.axis_size("gy")
    flags = jnp.pad(occupancy, ((1, 1), (1, 1), (0, 0)))
    window = lax.dynamic_slice(
        flags, (lax.axis_index("gx"), lax.axis_index("gy"), jnp.int32(0)), (3, 3, occupancy.shape[2]))
    mask = jnp.repeat(window, 8, axis=2).astype(F32)
    own = (features * mask[1, 1].astype(BF)).transpose(1, 2, 0, 3).reshape(N, N * C, Z)
    mask = jnp.pad(mask, ((0, 0), (0, 5), (0, 0)))
    pown = jnp.concatenate([grad_pooled, pool_choice.astype(BF)], axis=3)
    pown = pown.transpose(1, 2, 0, 3).reshape(Q, Q * C, Z)

    face = ((N * H + Q, C, Z), BF)
    ydown, yup, near, far = call(pack_faces, [face] * 4)(own, pown)
    ylow = shift(ydown, "gy", 1)
    yhigh = shift(yup, "gy", -1)
    xfar = swap(far, "gx", 1)
    xnear = swap(near, "gx", 0)

    def blocks(weight):
        return weight.transpose(1, 2, 3, 0, 4).reshape(27, C, C)

    t1, t2, f2, f1, b1, b2 = call(
        prepare, [((6 * C, 12 * C), BF)] * 4 + [((C, Z), F32)] * 2)(
            blocks(weight_one), blocks(weight_two),
            bias_one.reshape(1, C), bias_two.reshape(1, C))

    own, pown, t1 = lax.optimization_barrier((own, pown, t1))
    corner = ((N * H + 2, C, Z), BF)
    mfeat, mpool, near, far = call(
        pack_corners,
        [((N, W * C, Z), BF), ((Q, (Q + 2) * C, Z), BF)] + [corner] * 2)(own, pown, ylow, yhigh)
    cfar = swap(far, "gx", 1)
    cnear = swap(near, "gx", 0)

    grads = [((9 * C, 3 * C), F32)] * 2 + [((C, Z), F32)] * 2
    mids = call(
        middle,
        [((6, (W - 2) * C, Z), BF), ((4, (W - 4) * C, Z), BF), ((2, (W - 6) * C, Z), BF)] + grads,
        [((2, (Q + 2) * C, 2 * Z), F32)])(mfeat, mpool, mask, t1, t2, f2, b1, b2)

    rims = call(
        rim,
        [face, face, ((8, 6 * C, Z), BF), ((8, 4 * C, Z), BF), ((8, 2 * C, Z), BF)] + grads,
        [((4, (Q + 2) * C, 2 * Z), F32)])(mfeat, mpool, xnear, xfar, *mids, mask, t1, t2, f2, b1, b2)

    one, parts = call(
        outer, [((W - 6, (W - 6) * C, Z), BF), ((devices * ROWS, Z), BF)],
        [corner, corner, ((8, (W - 2) * C, Z), BF), ((8, (W - 4) * C, Z), BF),
         ((4, (Q + 2) * C, 2 * Z), F32)] + grads)(mfeat, mpool, cnear, cfar, *mids[:3], *rims, mask, t1, t2, f2, b1, b2)

    block = (devices, ROWS, Z)
    got = lax.all_to_all(parts.reshape(block), axes, 0, 0, tiled=True)
    out, = call(final, [((N, N * C, Z), BF)])(one, mask, f1)
    mine, = call(add_up, [(block, BF)])(got)
    summed = lax.all_to_all(mine, axes, 0, 0, tiled=True).reshape(devices * ROWS, Z)
    gw1, gw2, gb1, gb2 = call(
        unpack, [((27, C, C), F32)] * 2 + [((1, C), F32)] * 2)(summed)

    def weights(g):
        return g.reshape(3, 3, 3, C, C).transpose(3, 0, 1, 2, 4)

    grad_input = out.reshape(N, N, C, Z).transpose(2, 0, 1, 3)
    return grad_input, weights(gw1), gb1.reshape(C), weights(gw2), gb2.reshape(C)


def solution(mesh):
    cells = P(None, "gx", "gy", None)
    return jax.shard_map(
        steps,
        mesh=mesh,
        in_specs=(cells, P(), P(), P(), P(), P(), cells, cells),
        out_specs=(cells, P(), P(), P(), P()),
        check_vma=False,
    )
```

```python
import math

import jax
import jax.numpy as jnp
from jax import lax
from jax.experimental import pallas as pl
from jax.experimental.pallas import tpu as pltpu
from jax.sharding import PartitionSpec as P


BF = jnp.bfloat16
F32 = jnp.float32
C, Z, N, H = 32, 128, 8, 4
W = N + 2 * H
Q = N // 2
ROWS = 8
CELLS = 128 * 64 * 128


def call(kernel, outs, scratch=()):
    return pl.pallas_call(
        kernel,
        out_shape=tuple(jax.ShapeDtypeStruct(s, d) for s, d in outs),
        scratch_shapes=[pltpu.VMEM(s, d) for s, d in scratch],
        compiler_params=pltpu.CompilerParams(vmem_limit_bytes=40 << 20),
    )


def swap(v, axis, first):
    pairs = []
    for i in range(first, lax.axis_size(axis) - 1, 2):
        pairs += [(i, i + 1), (i + 1, i)]
    return lax.ppermute(v, axis, pairs)


def odd_place(axis="gx"):
    return lax.axis_index(axis) % 2


def cell(y, n=1):
    return slice(y * C, (y + n) * C)


def prepare(w1, w2, b1, b2, t1, t2, f2, f1, c1, c2):
    zero = jnp.zeros((C, C), F32)
    for src, plain, flip in ((w1, t1, f1), (w2, t2, f2)):
        for a in range(3):
            for c in range(3):
                rows = slice(c * C, (c + 1) * C)
                high = slice((3 + c) * C, (4 + c) * C)
                cols = slice(a * 4 * C, (a + 1) * 4 * C)
                line = jnp.concatenate(
                    [src[a * 9 + b * 3 + c].astype(F32) for b in range(3)] + [zero], axis=1)
                plain[rows, cols] = line.astype(BF)
                plain[high, cols] = pltpu.roll(line, C, 1).astype(BF)
                tall = jnp.concatenate(
                    [src[(2 - a) * 9 + (2 - b) * 3 + 2 - c].astype(F32) for b in range(3)] + [zero],
                    axis=0)
                line = jnp.transpose(tall)
                flip[rows, cols] = line.astype(BF)
                flip[high, cols] = pltpu.roll(line, C, 1).astype(BF)
    for src, dst in ((b1, c1), (b2, c2)):
        dst[...] = jnp.transpose(jnp.broadcast_to(src[...], (Z, C)))


def flags_around(occ, x, y):
    nx, ny, nz = occ.shape
    row = lax.broadcasted_iota(jnp.int32, (8, ny), 0)
    col = lax.broadcasted_iota(jnp.int32, (8, ny), 1)
    brick = lax.broadcasted_iota(jnp.int32, (nz, Z), 0)
    lane = lax.broadcasted_iota(jnp.int32, (nz, Z), 1)
    widen = jnp.where(lane // (Z // nz) == brick, 1.0, 0.0)
    out = []
    for d in range(3):
        at = x + d - 1
        inside = ((at >= 0) & (at < nx)).astype(F32)
        tile = occ[jnp.clip(at, 0, nx - 1)].astype(F32) * inside
        pick = jnp.where((col == row + y - 1) & (row < 3), 1.0, 0.0)
        near = jnp.dot(pick, tile, preferred_element_type=F32)
        out.append(jnp.dot(near, widen, preferred_element_type=F32))
    return out


def pack_faces(cells, grad, pick, occ, own, pown, mask, ynear, yfar, near, far):
    odd = odd_place()
    for d, flags in enumerate(flags_around(occ, lax.axis_index("gx"), lax.axis_index("gy"))):
        mask[d] = flags
    here = mask[1][1:2, :]
    for x in range(N):
        own[x] = (cells[x].astype(F32) * here).astype(BF)
    for x in range(Q):
        pown[x] = jnp.concatenate([grad[x].astype(F32), pick[x].astype(F32)], axis=1).astype(BF)

    def sides(low, high):
        for x in range(N):
            for k in range(H):
                high[x * H + k] = own[x, cell(N - H + k), :]
                low[x * H + k] = own[x, cell(k), :]
        for q in range(Q):
            high[N * H + q] = pown[q, cell(Q - 1), :]
            low[N * H + q] = pown[q, cell(0), :]

    @pl.when(odd_place("gy") == 0)
    def _():
        sides(yfar, ynear)

    @pl.when(odd_place("gy") == 1)
    def _():
        sides(ynear, yfar)

    for ref, low in ((near, odd), (far, 1 - odd)):
        for k in range(H):
            for y in range(N):
                ref[k * N + y] = own[(N - H) * (1 - low) + k, cell(y), :]
        for q in range(Q):
            ref[N * H + q] = pown[(Q - 1) * (1 - low), cell(q), :]


def pack_corners(own, pown, ynear, yfar, feat, pool, near, far, ylow, yhigh):
    resolve(ynear, yfar, ylow, yhigh, "gy")
    odd = odd_place()
    for ref, low in ((near, odd), (far, 1 - odd)):
        for x in range(H):
            for k in range(H):
                at = ((N - H) * (1 - low) + x) * H + k
                ref[x * N + k] = ylow[at]
                ref[x * N + H + k] = yhigh[at]
        at = N * H + (Q - 1) * (1 - low)
        ref[N * H] = ylow[at]
        ref[N * H + 1] = yhigh[at]
    for x in range(N):
        feat[x, cell(H, N), :] = own[x]
        for k in range(H):
            feat[x, cell(k), :] = ylow[x * H + k]
            feat[x, cell(H + N + k), :] = yhigh[x * H + k]
    for x in range(Q):
        pool[x, cell(1, Q), :] = pown[x]
        pool[x, cell(0), :] = ylow[N * H + x]
        pool[x, cell(Q + 1), :] = yhigh[N * H + x]


def after(v):
    lane = lax.broadcasted_iota(jnp.int32, v.shape, 1)
    return jnp.where(lane == 0, 0.0, pltpu.roll(v, 1, 1))


def before(v):
    lane = lax.broadcasted_iota(jnp.int32, v.shape, 1)
    return jnp.where(lane == Z - 1, 0.0, pltpu.roll(v, Z - 1, 1))


def spreader():
    row = lax.broadcasted_iota(jnp.int32, (Z, 2 * Z), 0)
    col = lax.broadcasted_iota(jnp.int32, (Z, 2 * Z), 1)
    return jnp.where(row == col // 2, 1.0, 0.0).astype(BF)


def conv_pair(rows_at, x, weight, pairs, write, i):
    for j in pairs:
        rows = [rows_at(x + d, 2 * j, 4) for d in range(4)]
        tile = jnp.concatenate(
            [jnp.concatenate([rows[d], rows[d + 1]], axis=1) for d in range(3)], axis=0)
        got = jnp.dot(weight[...], tile, preferred_element_type=F32)
        for xo in range(2):
            for yo in range(2):
                g = got[yo * 3 * C:(yo + 1) * 3 * C, xo * Z:(xo + 1) * Z]
                v = g[C:2 * C] + after(g[0:C]) + before(g[2 * C:])
                write(i, j, xo, yo, v)


def planes(ref, first=0):
    def rows_at(x, y, n=1):
        return ref[x - first, cell(y, n), :]

    return rows_at


def writers(mask, b1, b2, ups_at, hid_at, hid_put, two_put, one_put):
    lane = lax.broadcasted_iota(jnp.int32, (C, Z), 1)
    odd = (lane % 2).astype(F32)

    def mask_of(i, j, xo, yo, reach):
        bx = (2 * i + xo + N - reach) >> 3
        by = (2 * j + yo + N - reach) >> 3
        return mask[bx][by:by + 1, :]

    def write_hidden(i, j, xo, yo, v):
        m = mask_of(i, j, xo, yo, H - 1)
        hid_put(2 * i + xo, 2 * j + yo, (jnp.maximum(v + b1[...], 0.0) * m).astype(BF))

    def write_two(i, j, xo, yo, v):
        m = mask_of(i, j, xo, yo, H - 2)
        grad, pick = ups_at(i, j)
        live = (pick == odd + float(4 * xo + 2 * yo)) & (v + b2[...] > 0.0)
        two_put(2 * i + xo, 2 * j + yo, jnp.where(live, grad * m, 0.0).astype(BF))

    def write_one(i, j, xo, yo, v):
        h = hid_at(2 * i + xo + 2, 2 * j + yo + 2).astype(F32)
        one_put(2 * i + xo, 2 * j + yo, jnp.where(h > 0.0, v, 0.0).astype(BF))

    return write_hidden, write_two, write_one


def putter(ref, index):
    def put(x, y, v):
        ref[index(x), cell(y), :] = v

    return put


def upstream(ups, index):
    def ups_at(i, j):
        return ups[index(i), cell(j), 0:Z], ups[index(i), cell(j), Z:2 * Z]

    return ups_at


def term(x, ys, bias, src_at, off_s, delta_at, off_d, acc):
    rights = []
    for y in ys:
        d = delta_at(x + off_d, y + off_d).astype(F32)
        bias[...] += d
        rights.append(jnp.concatenate([before(d), d, after(d)], axis=0).astype(BF))
    left = jnp.concatenate(
        [jnp.concatenate([src_at(x + off_s + a, y + off_s, 3) for y in ys], axis=1)
         for a in range(3)], axis=0)
    acc[...] += lax.dot_general(left, jnp.concatenate(rights, axis=1), (((1,), (1,)), ((), ())),
                                preferred_element_type=F32)


def middle(feat, pool, mask, t1, t2, f2, b1, b2, hid, two, one, acc1, acc2, s1, s2, ups):
    spread = spreader()
    for p in range(2):
        ups[p] = jnp.dot(pool[1 + p], spread, preferred_element_type=F32)
    feat_at, hid_at, two_at, one_at = planes(feat, 4), planes(hid, 4), planes(two, 4), planes(one, 4)
    mid = lambda x: x - 4
    write_hidden, write_two, write_one = writers(
        mask, b1, b2, upstream(ups, lambda i: i - 2), hid_at,
        putter(hid, mid), putter(two, mid), putter(one, mid))
    for ref in (acc1, acc2, s1, s2):
        ref[...] = jnp.zeros_like(ref)
    for i in (2, 3, 4):
        conv_pair(feat_at, 2 * i, t1, range(W // 2 - 1), write_hidden, i)
    for i in (2, 3):
        conv_pair(hid_at, 2 * i, t2, range(W // 2 - 2), write_two, i)
    conv_pair(two_at, 4, f2, range(W // 2 - 3), write_one, 2)
    for x in range(2, 6):
        term(x, range(N), s2, hid_at, H - 2, two_at, H - 2, acc2)
    for x in range(3, 5):
        term(x, range(N), s1, feat_at, H - 1, one_at, H - 3, acc1)


def packed(x, mid):
    return x if x < 4 else x - mid


def merged(ref, full, mid, inner=None, count=0):
    def one_cell(p, y):
        if 4 <= y < 4 + count:
            return inner[p, cell(y - 4), :]
        return ref[p, cell(y), :]

    def rows_at(x, y, n=1):
        if 4 <= x < 4 + mid:
            return full[x - 4, cell(y, n), :]
        return jnp.concatenate([one_cell(packed(x, mid), v) for v in range(y, y + n)], axis=0)

    return rows_at


def features_at(mfeat, xlow, xhigh, clow, chigh):
    def feat_at(x, y, n=1):
        if H <= x < H + N:
            return mfeat[x - H, cell(y, n), :]
        side, corner, k = (xlow, clow, x) if x < H else (xhigh, chigh, x - H - N)
        cells = []
        for v in range(y, y + n):
            if H <= v < H + N:
                cells.append(side[k * N + v - H])
            else:
                cells.append(corner[k * N + (v if v < H else v - N)])
        return jnp.concatenate(cells, axis=0)

    return feat_at


def resolve(near, far, low, high, axis="gx"):
    odd = odd_place(axis)

    @pl.when(odd == 0)
    def _():
        low[...], high[...] = far[...], near[...]

    @pl.when(odd == 1)
    def _():
        low[...], high[...] = near[...], far[...]


def rim(mfeat, mpool, xnear, xfar, mhid, mtwo, mone, macc1, macc2, ms1, ms2, mask,
        t1, t2, f2, b1, b2, xlow, xhigh, hid, two, one, acc1, acc2, s1, s2, ups):
    resolve(xnear, xfar, xlow, xhigh)
    spread = spreader()
    for row, side in ((0, xlow), (3, xhigh)):
        for y in range(2, Q):
            ups[row, cell(y), :] = jnp.dot(
                side[N * H + y - 1], spread, preferred_element_type=F32)
    ups[1] = jnp.dot(mpool[0], spread, preferred_element_type=F32)
    ups[2] = jnp.dot(mpool[Q - 1], spread, preferred_element_type=F32)

    def inner_put(ref, mid):
        def put(x, y, v):
            ref[packed(x, mid), cell(y - 4), :] = v

        return put

    feat_at = features_at(mfeat, xlow, xhigh, None, None)
    hid_at = merged(None, mhid, 6, hid, 6)
    two_at = merged(None, mtwo, 4, two, 4)
    one_at = merged(None, mone, 2, one, 2)
    write_hidden, write_two, write_one = writers(
        mask, b1, b2, upstream(ups, lambda i: packed(i, 2) if i > 3 else i), hid_at,
        inner_put(hid, 6), inner_put(two, 4), inner_put(one, 2))
    for dst, src in ((acc1, macc1), (acc2, macc2), (s1, ms1), (s2, ms2)):
        dst[...] = src[...]
    for i in (0, 1, 5, 6):
        conv_pair(feat_at, 2 * i, t1, (2, 3, 4), write_hidden, i)
    for i in (0, 1, 4, 5):
        conv_pair(hid_at, 2 * i, t2, (2, 3), write_two, i)
    for i in (0, 1, 3, 4):
        conv_pair(two_at, 2 * i, f2, (2,), write_one, i)
    for x in (0, 1, 6, 7):
        term(x, (2, 3, 4, 5), s2, hid_at, H - 2, two_at, H - 2, acc2)
    for x in (0, 1, 2, 5, 6, 7):
        term(x, (3, 4), s1, feat_at, H - 1, one_at, H - 3, acc1)


def outer(mfeat, mpool, cnear, cfar, mhid, mtwo, mone, xlow, xhigh, rhid, rtwo, rone,
          macc1, macc2, ms1, ms2, mask, t1, t2, f2, b1, b2, one, parts,
          clow, chigh, hid, two, ups, acc1, acc2, s1, s2):
    resolve(cnear, cfar, clow, chigh)
    spread = spreader()
    for row, side, corner in ((0, xlow, clow), (3, xhigh, chigh)):
        for y in range(Q + 2):
            if 1 <= y <= Q:
                given = side[N * H + y - 1]
            else:
                given = corner[N * H + (y > 0)]
            ups[row, cell(y), :] = jnp.dot(given, spread, preferred_element_type=F32)
    ups[1] = jnp.dot(mpool[0], spread, preferred_element_type=F32)
    ups[2] = jnp.dot(mpool[Q - 1], spread, preferred_element_type=F32)

    def rim_put(ref, mid):
        return putter(ref, lambda x: packed(x, mid))

    feat_at = features_at(mfeat, xlow, xhigh, clow, chigh)
    hid_at = merged(hid, mhid, 6, rhid, 6)
    two_at = merged(two, mtwo, 4, rtwo, 4)
    one_at = planes(one)
    for x in range(10):
        if 4 <= x < 6:
            one[x] = mone[x - 4]
        else:
            one[x, cell(4, 2), :] = rone[packed(x, 2)]
    write_hidden, write_two, write_one = writers(
        mask, b1, b2, upstream(ups, lambda i: packed(i, 2) if i > 3 else i), hid_at,
        rim_put(hid, 6), rim_put(two, 4), putter(one, lambda x: x))
    acc1[...] = macc1[...]
    acc2[...] = macc2[...]
    s1[...] = ms1[...]
    s2[...] = ms2[...]
    for i in (0, 1, 5, 6):
        conv_pair(feat_at, 2 * i, t1, (0, 1, 5, 6), write_hidden, i)
    for i in (0, 1, 4, 5):
        conv_pair(hid_at, 2 * i, t2, (0, 1, 4, 5), write_two, i)
    for i in (0, 1, 3, 4):
        conv_pair(two_at, 2 * i, f2, (0, 1, 3, 4), write_one, i)
    for x in (0, 1, 6, 7):
        term(x, (0, 1, 6, 7), s2, hid_at, H - 2, two_at, H - 2, acc2)
    for x in (0, 1, 2, 5, 6, 7):
        term(x, (0, 1, 2, 5, 6, 7), s1, feat_at, H - 1, one_at, H - 3, acc1)
    rows9 = 9 * C
    pad = jnp.zeros((rows9, Z - 3 * C), F32)
    for k, (acc, sums) in enumerate(((acc1, s1), (acc2, s2))):
        parts[k * rows9:(k + 1) * rows9, :] = jnp.concatenate([acc[...], pad], axis=1).astype(BF)
        total = jnp.sum(sums[...], axis=1, keepdims=True)
        parts[2 * rows9 + k * C:2 * rows9 + (k + 1) * C, :] = jnp.broadcast_to(
            total, (C, Z)).astype(BF)
    rest = parts.shape[0] - 20 * C
    parts[20 * C:, :] = jnp.zeros((rest, Z), BF)


def add_up(got, out):
    total = jnp.sum(got[...].astype(F32), axis=0, keepdims=True).astype(BF)
    out[...] = jnp.broadcast_to(total, out.shape)


def unpack(summed, w1, w2, b1, b2):
    scale = 1.0 / math.sqrt(CELLS)
    rows9 = 9 * C
    for k, (w, b) in enumerate(((w1, b1), (w2, b2))):
        for n in range(9):
            rows = slice(k * rows9 + n * C, k * rows9 + (n + 1) * C)
            block = jnp.transpose(summed[rows, :].astype(F32) * scale)
            for c in range(3):
                w[n * 3 + c] = block[c * C:(c + 1) * C, :]
        rows = slice(2 * rows9 + k * C, 2 * rows9 + (k + 1) * C)
        b[...] = jnp.transpose(summed[rows, :].astype(F32) * scale)[0:1, :]


def final(one, mask, f1, out):
    def write_out(i, j, xo, yo, v):
        out[2 * i + xo, cell(2 * j + yo), :] = (v * mask[1][1:2, :]).astype(BF)

    for i in range(N // 2):
        conv_pair(planes(one), 2 * i, f1, range(N // 2), write_out, i)


def steps(features, occupancy, weight_one, bias_one, weight_two, bias_two, grad_pooled, pool_choice):
    axes = ("gx", "gy")
    devices = lax.axis_size("gx") * lax.axis_size("gy")

    def inner(v):
        return v.transpose(1, 2, 0, 3).reshape(v.shape[1], v.shape[2] * C, v.shape[3])

    face = ((N * H + Q, C, Z), BF)
    own, pown, mask, ynear, yfar, near, far = call(
        pack_faces, [((N, N * C, Z), BF), ((Q, Q * C, Z), BF), ((3, 8, Z), F32)] + [face] * 4)(inner(features), inner(grad_pooled), inner(pool_choice), occupancy)
    yfar = swap(yfar, "gy", 1)
    ynear = swap(ynear, "gy", 0)
    xfar = swap(far, "gx", 1)
    xnear = swap(near, "gx", 0)

    def blocks(weight):
        return weight.transpose(1, 2, 3, 0, 4).reshape(27, C, C)

    t1, t2, f2, f1, b1, b2 = call(
        prepare, [((6 * C, 12 * C), BF)] * 4 + [((C, Z), F32)] * 2)(
            blocks(weight_one), blocks(weight_two),
            bias_one.reshape(1, C), bias_two.reshape(1, C))

    own, pown, t1 = lax.optimization_barrier((own, pown, t1))
    corner = ((N * H + 2, C, Z), BF)
    mfeat, mpool, near, far = call(
        pack_corners,
        [((N, W * C, Z), BF), ((Q, (Q + 2) * C, Z), BF)] + [corner] * 2,
        [face, face])(own, pown, ynear, yfar)
    cfar = swap(far, "gx", 1)
    cnear = swap(near, "gx", 0)

    grads = [((9 * C, 3 * C), F32)] * 2 + [((C, Z), F32)] * 2
    mids = call(
        middle,
        [((6, (W - 2) * C, Z), BF), ((4, (W - 4) * C, Z), BF), ((2, (W - 6) * C, Z), BF)] + grads,
        [((2, (Q + 2) * C, 2 * Z), F32)])(mfeat, mpool, mask, t1, t2, f2, b1, b2)

    rims = call(
        rim,
        [face, face, ((8, 6 * C, Z), BF), ((8, 4 * C, Z), BF), ((8, 2 * C, Z), BF)] + grads,
        [((4, (Q + 2) * C, 2 * Z), F32)])(mfeat, mpool, xnear, xfar, *mids, mask, t1, t2, f2, b1, b2)

    one, parts = call(
        outer, [((W - 6, (W - 6) * C, Z), BF), ((devices * ROWS, Z), BF)],
        [corner, corner, ((8, (W - 2) * C, Z), BF), ((8, (W - 4) * C, Z), BF),
         ((4, (Q + 2) * C, 2 * Z), F32)] + grads)(mfeat, mpool, cnear, cfar, *mids[:3], *rims, mask, t1, t2, f2, b1, b2)

    block = (devices, ROWS, Z)
    got = lax.all_to_all(parts.reshape(block), axes, 0, 0, tiled=True)
    out, = call(final, [((N, N * C, Z), BF)])(one, mask, f1)
    mine, = call(add_up, [(block, BF)])(got)
    summed = lax.all_to_all(mine, axes, 0, 0, tiled=True).reshape(devices * ROWS, Z)
    gw1, gw2, gb1, gb2 = call(
        unpack, [((27, C, C), F32)] * 2 + [((1, C), F32)] * 2)(summed)

    def weights(g):
        return g.reshape(3, 3, 3, C, C).transpose(3, 0, 1, 2, 4)

    grad_input = out.reshape(N, N, C, Z).transpose(2, 0, 1, 3)
    return grad_input, weights(gw1), gb1.reshape(C), weights(gw2), gb2.reshape(C)


def solution(mesh):
    cells = P(None, "gx", "gy", None)
    return jax.shard_map(
        steps,
        mesh=mesh,
        in_specs=(cells, P(), P(), P(), P(), P(), cells, cells),
        out_specs=(cells, P(), P(), P(), P()),
        check_vma=False,
    )
```

```python
import math

import jax
import jax.numpy as jnp
from jax import lax
from jax.experimental import pallas as pl
from jax.experimental.pallas import tpu as pltpu
from jax.sharding import PartitionSpec as P


BF = jnp.bfloat16
F32 = jnp.float32
C, Z, N, H = 32, 128, 8, 4
W = N + 2 * H
Q = N // 2
ROWS = 8
CELLS = 128 * 64 * 128


def call(kernel, outs, scratch=()):
    return pl.pallas_call(
        kernel,
        out_shape=tuple(jax.ShapeDtypeStruct(s, d) for s, d in outs),
        scratch_shapes=[pltpu.VMEM(s, d) for s, d in scratch],
        compiler_params=pltpu.CompilerParams(vmem_limit_bytes=40 << 20),
    )


def swap(v, axis, first):
    pairs = []
    for i in range(first, lax.axis_size(axis) - 1, 2):
        pairs += [(i, i + 1), (i + 1, i)]
    return lax.ppermute(v, axis, pairs)


def odd_place(axis="gx"):
    return lax.axis_index(axis) % 2


def cell(y, n=1):
    return slice(y * C, (y + n) * C)


def prepare(w1, w2, t1, t2, f2, f1):
    zero = jnp.zeros((C, C), F32)
    for src, plain, flip in ((w1, t1, f1), (w2, t2, f2)):
        for a in range(3):
            for c in range(3):
                rows = slice(c * C, (c + 1) * C)
                high = slice((3 + c) * C, (4 + c) * C)
                cols = slice(a * 4 * C, (a + 1) * 4 * C)
                line = jnp.concatenate(
                    [src[a * 9 + b * 3 + c].astype(F32) for b in range(3)] + [zero], axis=1)
                plain[rows, cols] = line.astype(BF)
                plain[high, cols] = pltpu.roll(line, C, 1).astype(BF)
                tall = jnp.concatenate(
                    [src[(2 - a) * 9 + (2 - b) * 3 + 2 - c].astype(F32) for b in range(3)] + [zero],
                    axis=0)
                line = jnp.transpose(tall)
                flip[rows, cols] = line.astype(BF)
                flip[high, cols] = pltpu.roll(line, C, 1).astype(BF)


def flags_around(occ, x, y):
    nx, ny, nz = occ.shape
    row = lax.broadcasted_iota(jnp.int32, (8, ny), 0)
    col = lax.broadcasted_iota(jnp.int32, (8, ny), 1)
    brick = lax.broadcasted_iota(jnp.int32, (nz, Z), 0)
    lane = lax.broadcasted_iota(jnp.int32, (nz, Z), 1)
    widen = jnp.where(lane // (Z // nz) == brick, 1.0, 0.0)
    out = []
    for d in range(3):
        at = x + d - 1
        inside = ((at >= 0) & (at < nx)).astype(F32)
        tile = occ[jnp.clip(at, 0, nx - 1)].astype(F32) * inside
        pick = jnp.where((col == row + y - 1) & (row < 3), 1.0, 0.0)
        near = jnp.dot(pick, tile, preferred_element_type=F32)
        out.append(jnp.dot(near, widen, preferred_element_type=F32))
    return out


def pack_faces(cells, grad, pick, occ, b1, b2,
               own, pown, mask, c1, c2, ynear, yfar, near, far):
    odd = odd_place()
    for d, flags in enumerate(flags_around(occ, lax.axis_index("gx"), lax.axis_index("gy"))):
        mask[d] = flags
    for src, dst in ((b1, c1), (b2, c2)):
        dst[...] = jnp.transpose(jnp.broadcast_to(src[...], (Z, C)))
    here = mask[1][1:2, :]
    for x in range(N):
        own[x] = (cells[x].astype(F32) * here).astype(BF)
    for x in range(Q):
        pown[x] = jnp.concatenate([grad[x].astype(F32), pick[x].astype(F32)], axis=1).astype(BF)

    def sides(low, high):
        for x in range(N):
            for k in range(H):
                high[x * H + k] = own[x, cell(N - H + k), :]
                low[x * H + k] = own[x, cell(k), :]
        for q in range(Q):
            high[N * H + q] = pown[q, cell(Q - 1), :]
            low[N * H + q] = pown[q, cell(0), :]

    @pl.when(odd_place("gy") == 0)
    def _():
        sides(yfar, ynear)

    @pl.when(odd_place("gy") == 1)
    def _():
        sides(ynear, yfar)

    for ref, low in ((near, odd), (far, 1 - odd)):
        for k in range(H):
            for y in range(N):
                ref[k * N + y] = own[(N - H) * (1 - low) + k, cell(y), :]
        for q in range(Q):
            ref[N * H + q] = pown[(Q - 1) * (1 - low), cell(q), :]


def pack_corners(own, pown, ynear, yfar, feat, pool, near, far, ylow, yhigh):
    resolve(ynear, yfar, ylow, yhigh, "gy")
    odd = odd_place()
    for ref, low in ((near, odd), (far, 1 - odd)):
        for x in range(H):
            for k in range(H):
                at = ((N - H) * (1 - low) + x) * H + k
                ref[x * N + k] = ylow[at]
                ref[x * N + H + k] = yhigh[at]
        at = N * H + (Q - 1) * (1 - low)
        ref[N * H] = ylow[at]
        ref[N * H + 1] = yhigh[at]
    for x in range(N):
        feat[x, cell(H, N), :] = own[x]
        for k in range(H):
            feat[x, cell(k), :] = ylow[x * H + k]
            feat[x, cell(H + N + k), :] = yhigh[x * H + k]
    for x in range(Q):
        pool[x, cell(1, Q), :] = pown[x]
        pool[x, cell(0), :] = ylow[N * H + x]
        pool[x, cell(Q + 1), :] = yhigh[N * H + x]


def after(v):
    lane = lax.broadcasted_iota(jnp.int32, v.shape, 1)
    return jnp.where(lane == 0, 0.0, pltpu.roll(v, 1, 1))


def before(v):
    lane = lax.broadcasted_iota(jnp.int32, v.shape, 1)
    return jnp.where(lane == Z - 1, 0.0, pltpu.roll(v, Z - 1, 1))


def spreader():
    row = lax.broadcasted_iota(jnp.int32, (Z, 2 * Z), 0)
    col = lax.broadcasted_iota(jnp.int32, (Z, 2 * Z), 1)
    return jnp.where(row == col // 2, 1.0, 0.0).astype(BF)


def conv_pair(rows_at, x, weight, pairs, write, i):
    for j in pairs:
        rows = [rows_at(x + d, 2 * j, 4) for d in range(4)]
        tile = jnp.concatenate(
            [jnp.concatenate([rows[d], rows[d + 1]], axis=1) for d in range(3)], axis=0)
        got = jnp.dot(weight[...], tile, preferred_element_type=F32)
        for xo in range(2):
            for yo in range(2):
                g = got[yo * 3 * C:(yo + 1) * 3 * C, xo * Z:(xo + 1) * Z]
                v = g[C:2 * C] + after(g[0:C]) + before(g[2 * C:])
                write(i, j, xo, yo, v)


def planes(ref, first=0):
    def rows_at(x, y, n=1):
        return ref[x - first, cell(y, n), :]

    return rows_at


def writers(mask, b1, b2, ups_at, hid_at, hid_put, two_put, one_put):
    lane = lax.broadcasted_iota(jnp.int32, (C, Z), 1)
    odd = (lane % 2).astype(F32)

    def mask_of(i, j, xo, yo, reach):
        bx = (2 * i + xo + N - reach) >> 3
        by = (2 * j + yo + N - reach) >> 3
        return mask[bx][by:by + 1, :]

    def write_hidden(i, j, xo, yo, v):
        m = mask_of(i, j, xo, yo, H - 1)
        hid_put(2 * i + xo, 2 * j + yo, (jnp.maximum(v + b1[...], 0.0) * m).astype(BF))

    def write_two(i, j, xo, yo, v):
        m = mask_of(i, j, xo, yo, H - 2)
        grad, pick = ups_at(i, j)
        live = (pick == odd + float(4 * xo + 2 * yo)) & (v + b2[...] > 0.0)
        two_put(2 * i + xo, 2 * j + yo, jnp.where(live, grad * m, 0.0).astype(BF))

    def write_one(i, j, xo, yo, v):
        h = hid_at(2 * i + xo + 2, 2 * j + yo + 2).astype(F32)
        one_put(2 * i + xo, 2 * j + yo, jnp.where(h > 0.0, v, 0.0).astype(BF))

    return write_hidden, write_two, write_one


def putter(ref, index):
    def put(x, y, v):
        ref[index(x), cell(y), :] = v

    return put


def upstream(ups, index):
    def ups_at(i, j):
        return ups[index(i), cell(j), 0:Z], ups[index(i), cell(j), Z:2 * Z]

    return ups_at


def term(x, ys, bias, src_at, off_s, delta_at, off_d, acc):
    rights = []
    for y in ys:
        d = delta_at(x + off_d, y + off_d).astype(F32)
        bias[...] += d
        rights.append(jnp.concatenate([before(d), d, after(d)], axis=0).astype(BF))
    left = jnp.concatenate(
        [jnp.concatenate([src_at(x + off_s + a, y + off_s, 3) for y in ys], axis=1)
         for a in range(3)], axis=0)
    acc[...] += lax.dot_general(left, jnp.concatenate(rights, axis=1), (((1,), (1,)), ((), ())),
                                preferred_element_type=F32)


def middle(feat, pool, mask, t1, t2, f2, b1, b2, hid, two, one, acc1, acc2, s1, s2, ups):
    spread = spreader()
    for p in range(2):
        ups[p] = jnp.dot(pool[1 + p], spread, preferred_element_type=F32)
    feat_at, hid_at, two_at, one_at = planes(feat, 4), planes(hid, 4), planes(two, 4), planes(one, 4)
    mid = lambda x: x - 4
    write_hidden, write_two, write_one = writers(
        mask, b1, b2, upstream(ups, lambda i: i - 2), hid_at,
        putter(hid, mid), putter(two, mid), putter(one, mid))
    for ref in (acc1, acc2, s1, s2):
        ref[...] = jnp.zeros_like(ref)
    for i in (2, 3, 4):
        conv_pair(feat_at, 2 * i, t1, range(W // 2 - 1), write_hidden, i)
    for i in (2, 3):
        conv_pair(hid_at, 2 * i, t2, range(W // 2 - 2), write_two, i)
    conv_pair(two_at, 4, f2, range(W // 2 - 3), write_one, 2)
    for x in range(2, 6):
        term(x, range(N), s2, hid_at, H - 2, two_at, H - 2, acc2)
    for x in range(3, 5):
        term(x, range(N), s1, feat_at, H - 1, one_at, H - 3, acc1)


def packed(x, mid):
    return x if x < 4 else x - mid


def merged(ref, full, mid, inner=None, count=0):
    def one_cell(p, y):
        if 4 <= y < 4 + count:
            return inner[p, cell(y - 4), :]
        return ref[p, cell(y), :]

    def rows_at(x, y, n=1):
        if 4 <= x < 4 + mid:
            return full[x - 4, cell(y, n), :]
        return jnp.concatenate([one_cell(packed(x, mid), v) for v in range(y, y + n)], axis=0)

    return rows_at


def features_at(mfeat, xlow, xhigh, clow, chigh):
    def feat_at(x, y, n=1):
        if H <= x < H + N:
            return mfeat[x - H, cell(y, n), :]
        side, corner, k = (xlow, clow, x) if x < H else (xhigh, chigh, x - H - N)
        cells = []
        for v in range(y, y + n):
            if H <= v < H + N:
                cells.append(side[k * N + v - H])
            else:
                cells.append(corner[k * N + (v if v < H else v - N)])
        return jnp.concatenate(cells, axis=0)

    return feat_at


def resolve(near, far, low, high, axis="gx"):
    odd = odd_place(axis)

    @pl.when(odd == 0)
    def _():
        low[...], high[...] = far[...], near[...]

    @pl.when(odd == 1)
    def _():
        low[...], high[...] = near[...], far[...]


def rim(mfeat, mpool, xnear, xfar, mhid, mtwo, mone, macc1, macc2, ms1, ms2, mask,
        t1, t2, f2, b1, b2, xlow, xhigh, hid, two, one, acc1, acc2, s1, s2, ups):
    resolve(xnear, xfar, xlow, xhigh)
    spread = spreader()
    for row, side in ((0, xlow), (3, xhigh)):
        for y in range(2, Q):
            ups[row, cell(y), :] = jnp.dot(
                side[N * H + y - 1], spread, preferred_element_type=F32)
    ups[1] = jnp.dot(mpool[0], spread, preferred_element_type=F32)
    ups[2] = jnp.dot(mpool[Q - 1], spread, preferred_element_type=F32)

    def inner_put(ref, mid):
        def put(x, y, v):
            ref[packed(x, mid), cell(y - 4), :] = v

        return put

    feat_at = features_at(mfeat, xlow, xhigh, None, None)
    hid_at = merged(None, mhid, 6, hid, 6)
    two_at = merged(None, mtwo, 4, two, 4)
    one_at = merged(None, mone, 2, one, 2)
    write_hidden, write_two, write_one = writers(
        mask, b1, b2, upstream(ups, lambda i: packed(i, 2) if i > 3 else i), hid_at,
        inner_put(hid, 6), inner_put(two, 4), inner_put(one, 2))
    for dst, src in ((acc1, macc1), (acc2, macc2), (s1, ms1), (s2, ms2)):
        dst[...] = src[...]
    for i in (0, 1, 5, 6):
        conv_pair(feat_at, 2 * i, t1, (2, 3, 4), write_hidden, i)
    for i in (0, 1, 4, 5):
        conv_pair(hid_at, 2 * i, t2, (2, 3), write_two, i)
    for i in (0, 1, 3, 4):
        conv_pair(two_at, 2 * i, f2, (2,), write_one, i)
    for x in (0, 1, 6, 7):
        term(x, (2, 3, 4, 5), s2, hid_at, H - 2, two_at, H - 2, acc2)
    for x in (0, 1, 2, 5, 6, 7):
        term(x, (3, 4), s1, feat_at, H - 1, one_at, H - 3, acc1)


def outer(mfeat, mpool, cnear, cfar, mhid, mtwo, mone, xlow, xhigh, rhid, rtwo, rone,
          macc1, macc2, ms1, ms2, mask, t1, t2, f2, b1, b2, one, parts,
          clow, chigh, hid, two, ups, acc1, acc2, s1, s2):
    resolve(cnear, cfar, clow, chigh)
    spread = spreader()
    for row, side, corner in ((0, xlow, clow), (3, xhigh, chigh)):
        for y in range(Q + 2):
            if 1 <= y <= Q:
                given = side[N * H + y - 1]
            else:
                given = corner[N * H + (y > 0)]
            ups[row, cell(y), :] = jnp.dot(given, spread, preferred_element_type=F32)
    ups[1] = jnp.dot(mpool[0], spread, preferred_element_type=F32)
    ups[2] = jnp.dot(mpool[Q - 1], spread, preferred_element_type=F32)

    def rim_put(ref, mid):
        return putter(ref, lambda x: packed(x, mid))

    feat_at = features_at(mfeat, xlow, xhigh, clow, chigh)
    hid_at = merged(hid, mhid, 6, rhid, 6)
    two_at = merged(two, mtwo, 4, rtwo, 4)
    one_at = planes(one)
    for x in range(10):
        if 4 <= x < 6:
            one[x] = mone[x - 4]
        else:
            one[x, cell(4, 2), :] = rone[packed(x, 2)]
    write_hidden, write_two, write_one = writers(
        mask, b1, b2, upstream(ups, lambda i: packed(i, 2) if i > 3 else i), hid_at,
        rim_put(hid, 6), rim_put(two, 4), putter(one, lambda x: x))
    acc1[...] = macc1[...]
    acc2[...] = macc2[...]
    s1[...] = ms1[...]
    s2[...] = ms2[...]
    for i in (0, 1, 5, 6):
        conv_pair(feat_at, 2 * i, t1, (0, 1, 5, 6), write_hidden, i)
    for i in (0, 1, 4, 5):
        conv_pair(hid_at, 2 * i, t2, (0, 1, 4, 5), write_two, i)
    for i in (0, 1, 3, 4):
        conv_pair(two_at, 2 * i, f2, (0, 1, 3, 4), write_one, i)
    for x in (0, 1, 6, 7):
        term(x, (0, 1, 6, 7), s2, hid_at, H - 2, two_at, H - 2, acc2)
    for x in (0, 1, 2, 5, 6, 7):
        term(x, (0, 1, 2, 5, 6, 7), s1, feat_at, H - 1, one_at, H - 3, acc1)
    rows9 = 9 * C
    pad = jnp.zeros((rows9, Z - 3 * C), F32)
    for k, (acc, sums) in enumerate(((acc1, s1), (acc2, s2))):
        parts[k * rows9:(k + 1) * rows9, :] = jnp.concatenate([acc[...], pad], axis=1).astype(BF)
        total = jnp.sum(sums[...], axis=1, keepdims=True)
        parts[2 * rows9 + k * C:2 * rows9 + (k + 1) * C, :] = jnp.broadcast_to(
            total, (C, Z)).astype(BF)
    rest = parts.shape[0] - 20 * C
    parts[20 * C:, :] = jnp.zeros((rest, Z), BF)


def add_up(got, out):
    total = jnp.sum(got[...].astype(F32), axis=0)
    total = total[:ROWS] + total[ROWS:]
    pair = jnp.concatenate([total, total], axis=0).astype(BF)
    out[...] = jnp.broadcast_to(pair[None], out.shape)


def unpack(summed, w1, w2, b1, b2):
    scale = 1.0 / math.sqrt(CELLS)
    rows9 = 9 * C
    for k, (w, b) in enumerate(((w1, b1), (w2, b2))):
        for n in range(9):
            rows = slice(k * rows9 + n * C, k * rows9 + (n + 1) * C)
            block = jnp.transpose(summed[rows, :].astype(F32) * scale)
            for c in range(3):
                w[n * 3 + c] = block[c * C:(c + 1) * C, :]
        rows = slice(2 * rows9 + k * C, 2 * rows9 + (k + 1) * C)
        b[...] = jnp.transpose(summed[rows, :].astype(F32) * scale)[0:1, :]


def final(one, mask, f1, out):
    def write_out(i, j, xo, yo, v):
        out[2 * i + xo, cell(2 * j + yo), :] = (v * mask[1][1:2, :]).astype(BF)

    for i in range(N // 2):
        conv_pair(planes(one), 2 * i, f1, range(N // 2), write_out, i)


def steps(features, occupancy, weight_one, bias_one, weight_two, bias_two, grad_pooled, pool_choice):
    axes = ("gx", "gy")
    devices = lax.axis_size("gx") * lax.axis_size("gy")

    def inner(v):
        return v.transpose(1, 2, 0, 3).reshape(v.shape[1], v.shape[2] * C, v.shape[3])

    face = ((N * H + Q, C, Z), BF)
    own, pown, mask, b1, b2, ynear, yfar, near, far = call(
        pack_faces,
        [((N, N * C, Z), BF), ((Q, Q * C, Z), BF), ((3, 8, Z), F32)] + [((C, Z), F32)] * 2
        + [face] * 4)(inner(features), inner(grad_pooled), inner(pool_choice), occupancy,
                      bias_one.reshape(1, C), bias_two.reshape(1, C))
    yfar = swap(yfar, "gy", 1)
    ynear = swap(ynear, "gy", 0)
    xfar = swap(far, "gx", 1)
    xnear = swap(near, "gx", 0)

    def blocks(weight):
        return weight.transpose(1, 2, 3, 0, 4).reshape(27, C, C)

    t1, t2, f2, f1 = call(prepare, [((6 * C, 12 * C), BF)] * 4)(
        blocks(weight_one), blocks(weight_two))

    own, pown, t1 = lax.optimization_barrier((own, pown, t1))
    corner = ((N * H + 2, C, Z), BF)
    mfeat, mpool, near, far = call(
        pack_corners,
        [((N, W * C, Z), BF), ((Q, (Q + 2) * C, Z), BF)] + [corner] * 2,
        [face, face])(own, pown, ynear, yfar)
    cfar = swap(far, "gx", 1)
    cnear = swap(near, "gx", 0)

    grads = [((9 * C, 3 * C), F32)] * 2 + [((C, Z), F32)] * 2
    mids = call(
        middle,
        [((6, (W - 2) * C, Z), BF), ((4, (W - 4) * C, Z), BF), ((2, (W - 6) * C, Z), BF)] + grads,
        [((2, (Q + 2) * C, 2 * Z), F32)])(mfeat, mpool, mask, t1, t2, f2, b1, b2)

    rims = call(
        rim,
        [face, face, ((8, 6 * C, Z), BF), ((8, 4 * C, Z), BF), ((8, 2 * C, Z), BF)] + grads,
        [((4, (Q + 2) * C, 2 * Z), F32)])(mfeat, mpool, xnear, xfar, *mids, mask, t1, t2, f2, b1, b2)

    one, parts = call(
        outer, [((W - 6, (W - 6) * C, Z), BF), ((devices * ROWS, Z), BF)],
        [corner, corner, ((8, (W - 2) * C, Z), BF), ((8, (W - 4) * C, Z), BF),
         ((4, (Q + 2) * C, 2 * Z), F32)] + grads)(mfeat, mpool, cnear, cfar, *mids[:3], *rims, mask, t1, t2, f2, b1, b2)

    block = (devices, ROWS, Z)
    got = lax.all_to_all(parts.reshape(block), axes, 0, 0, tiled=True)
    out, = call(final, [((N, N * C, Z), BF)])(one, mask, f1)
    tiles = (devices // 2, 2 * ROWS, Z)
    mine, = call(add_up, [(tiles, BF)])(got.reshape(tiles))
    summed = lax.all_to_all(mine.reshape(block), axes, 0, 0, tiled=True).reshape(devices * ROWS, Z)
    gw1, gw2, gb1, gb2 = call(
        unpack, [((27, C, C), F32)] * 2 + [((1, C), F32)] * 2)(summed)

    def weights(g):
        return g.reshape(3, 3, 3, C, C).transpose(3, 0, 1, 2, 4)

    grad_input = out.reshape(N, N, C, Z).transpose(2, 0, 1, 3)
    return grad_input, weights(gw1), gb1.reshape(C), weights(gw2), gb2.reshape(C)


def solution(mesh):
    cells = P(None, "gx", "gy", None)
    return jax.shard_map(
        steps,
        mesh=mesh,
        in_specs=(cells, P(), P(), P(), P(), P(), cells, cells),
        out_specs=(cells, P(), P(), P(), P()),
        check_vma=False,
    )
```
